32 devices in a mesh: child: 4 (over y, x), tile: 8 (over z, core).
Axes of the slice: x: 2, y: 2, z: 4, core: 2. Of those that a mesh axis runs over, the one named last changes fastest.
Arguments:
- child_tiles: bfloat16 [4, 128, 512, 512], P('child', 'tile'), may hold values from -6 to 6
- panel: bfloat16 [4, 4096, 512], P('child', 'tile'), may hold values from -1 to 1
- bases: bfloat16 [4, 4096, 128], P('child', 'tile'), may hold values from -0.25 to 0.25
- tile_blocks: int32 [4, 128, 2], P('child'), may hold values from 0 to 7, as said below
- tile_dest: int32 [4, 128, 1], P('child'), may hold values from 0 to 7; in each aligned block of 16 rows (0 to 15, 16 to 31, ..., all dimensions but the last counted through in order) at most 2 rows name the same one
- tile_slot: int32 [4, 128], P('child'), may hold values from 0 to 7
- parent_tiles: bfloat16 [4, 64, 512, 512], P('child', 'tile'), may hold values from -6 to 6
- parent_blocks: int32 [4, 64, 2], P('child', 'tile'), may hold values from 0 to 7, as said below
- sketch_test: bfloat16 [4096, 128], replicated, may hold values from -0.25 to 0.25
Outputs:
- updated_tiles: bfloat16 [4, 64, 512, 512], P('child', 'tile')
- row_sketch: float32 [4096, 128], P(('child', 'tile'))
The draws below stay inside these ranges and needn't reach their ends.
Inputs may be any that keep to these rules, and one draw needn't show every extreme that they name: `tile_blocks`: each tile's row block is not below its column block. `tile_dest`: among the tiles of one device (aligned blocks of 16 tiles of a child), at most 2 name the same owner. `parent_blocks`: each parent tile's row block is not below its column block.
All inputs are finite; a program needn't handle non-finite values.
Results may differ from the reference program's by a relative error of at most 0.0063.
Values may be sent and summed in bfloat16 or wider, within the bound.
No kernel may reach another device: no remote copies, remote signals or barrier semaphores. Data moves between devices by JAX's collectives and lax.ppermute only.
A program may use at most 192 MiB of HBM per device.

```python
import math
import jax
import jax.numpy as jnp
import numpy as np
from jax import lax

TILE = 512
RANK = 128
SKETCH = 128
TILES_DEV = 16
PARENT_DEV = 8
CAP = 2
BLOCKS = 8
PBLOCKS = 8
TILES = 128
PTILES = 64
N_CHILD = 4
N_TILE = 8


def draw_tile_blocks(key, part):
    first_key, second_key = jax.random.split(jax.random.fold_in(key, 11))
    row_ids = jax.random.randint(first_key, (N_CHILD, TILES, 1), 0, BLOCKS)
    col_ids = jax.random.randint(second_key, (N_CHILD, TILES, 1), 0, row_ids + 1)
    return jnp.concatenate([row_ids, col_ids], axis=2).astype(jnp.int32)


def draw_parent_blocks(key, part):
    first_key, second_key = jax.random.split(jax.random.fold_in(key, 23))
    row_ids = jax.random.randint(first_key, (N_CHILD, PTILES, 1), 0, PBLOCKS)
    col_ids = jax.random.randint(second_key, (N_CHILD, PTILES, 1), 0, row_ids + 1)
    return jnp.concatenate([row_ids, col_ids], axis=2).astype(jnp.int32)


def plant(values, rng, low, top_value):
    longest = values.shape.index(max(values.shape))
    spots = []
    for shift in (0, 1):
        where = [jax.random.randint(jax.random.fold_in(rng, axis), (), 0, length) for axis, length in enumerate(values.shape)]
        where[longest] = (where[longest] + shift) % values.shape[longest]
        spots.append(tuple(where))
    return values.at[spots[0]].set(low).at[spots[1]].set(top_value)


def shard_levels(stream_key, shape, shards, smallest, largest):
    def one(position, blocks):
        draws = jax.random.uniform(jax.random.fold_in(jax.random.fold_in(stream_key, 6), position), (blocks,), jnp.float32, smallest / len(shards), largest / len(shards))
        return jnp.repeat(jnp.exp(draws), shape[position] // blocks).reshape((-1,) + (1,) * (len(shape) - position - 1))

    factor_of = one(*shards[0])
    for cut in shards[1:]:
        factor_of = factor_of * one(*cut)
    return factor_of


def routed_block(rng, own, number, rows, count, top, bound, skew):
    sequence = jax.random.permutation(rng, count)
    heavy_load, common = shares(count, rows * top, bound, skew, True), shares(count, rows * top, bound, skew, False)
    places = jnp.arange(count)

    def named(sizes, turn):
        used = int((sizes > 0).sum())
        fixed = max(1, used // 4)
        passed = fixed + (places - fixed + turn * (used - fixed)) % max(1, count - fixed)
        return jnp.zeros((count,), jnp.int32).at[sequence[jnp.where(places < fixed, places, passed)]].set(jnp.asarray(sizes, jnp.int32))

    sizes = jnp.where(number % 4 == 0, named(heavy_load, number // 4), named(common, number - number // 4 - 1))
    mixed = jax.random.permutation(jax.random.fold_in(own, 3), count)
    source_of, taker = mixed[0:count // 2 * 2:2], mixed[1:count // 2 * 2:2]
    room = jnp.minimum(sizes[source_of] - 1, bound - sizes[taker]) // 2
    room = jnp.where((source_of == sequence[0]) | (taker == sequence[0]) | (sizes[taker] == 0), 0, jnp.maximum(room, 0))
    passed = jax.random.randint(jax.random.fold_in(own, 4), (count // 2,), 0, 1 << 20) % (room + 1)
    sizes = sizes.at[source_of].add(-passed).at[taker].add(passed)
    labels = jnp.searchsorted(jnp.cumsum(sizes), jnp.arange(rows * top), side="right").astype(jnp.int32)
    grid = labels.reshape(top, rows).T
    grid = grid[jax.random.permutation(jax.random.fold_in(own, 1), rows)]
    turn = jax.random.randint(jax.random.fold_in(own, 2), (rows, 1), 0, top)
    return jnp.take_along_axis(grid, (jnp.arange(top)[None, :] + turn) % top, axis=1)


def shares(number_of, total, bound, slope, full):
    loads = [(1 << 20) // math.isqrt(rank ** slope) + 1 for rank in range(1, number_of + 1)]
    largest = bound if full else min(bound, max(-(-total // number_of), total * loads[0] // sum(loads)))
    least = 1 if total - largest >= number_of - 1 else 0
    given, rest = [largest] + [least] * (number_of - 1), total - largest - least * (number_of - 1)
    while rest > 0:
        candidates = [i for i in range(1, number_of) if given[i] < largest] or [i for i in range(1, number_of) if given[i] < bound]
        mass, budget = sum([loads[i] for i in candidates]), rest
        for i in candidates:
            addition = min(bound - given[i], max(1, budget * loads[i] // mass), rest)
            given[i] = given[i] + addition
            rest = rest - addition
    return np.array(given)


def normal_values(own_key, dims, deviation, reach, shards=(), dtype=jnp.bfloat16):
    level = shard_levels(own_key, dims, shards, -0.22, 0.18) if shards else 1.0
    result = jax.random.normal(own_key, dims, jnp.float32) * deviation * level
    return jnp.minimum(jnp.maximum(result, -reach), reach).astype(dtype)


def setup_inputs(seed: int = 0) -> dict:
    key_of = jax.random.split(jax.random.key(seed), 10)
    child_tiles = normal_values(key_of[0], (N_CHILD, TILES, TILE, TILE), 1.0, 6.0, ((0, 4), (1, 8)))
    panel = normal_values(key_of[1], (N_CHILD, BLOCKS * TILE, TILE), 0.21, 1.0, ((0, 4), (1, 8)))
    bases = normal_values(key_of[2], (N_CHILD, BLOCKS * TILE, RANK), TILE ** -0.5, 0.25, ((0, 4), (1, 8)))
    tile_blocks = draw_tile_blocks(jax.random.fold_in(key_of[9], 71), 0)
    tile_dest_keys = jax.random.split(jax.random.fold_in(key_of[4], 1), N_CHILD * TILES // TILES_DEV)
    tile_dest_turns = jax.random.permutation(jax.random.fold_in(key_of[4], 3), N_CHILD * TILES // TILES_DEV)
    tile_dest = jax.vmap(lambda own, number: routed_block(jax.random.fold_in(key_of[4], 2), own, number, TILES_DEV, N_TILE, 1, CAP, 2))(tile_dest_keys, tile_dest_turns).reshape((N_CHILD, TILES, 1))
    tile_slot = plant(jax.random.randint(key_of[5], (N_CHILD, TILES), 0, PARENT_DEV), jax.random.fold_in(key_of[5], 1), 0, PARENT_DEV - 1).astype(jnp.int32)
    parent_tiles = normal_values(key_of[6], (N_CHILD, PTILES, TILE, TILE), 1.0, 6.0, ((0, 4), (1, 8)))
    parent_blocks = draw_parent_blocks(jax.random.fold_in(key_of[9], 71), 0)
    sketch_test = normal_values(key_of[8], (PBLOCKS * TILE, SKETCH), TILE ** -0.5, 0.25)
    return {"child_tiles": child_tiles, "panel": panel, "bases": bases, "tile_blocks": tile_blocks, "tile_dest": tile_dest, "tile_slot": tile_slot, "parent_tiles": parent_tiles, "parent_blocks": parent_blocks, "sketch_test": sketch_test}


def reference(child_tiles, panel, bases, tile_blocks, tile_dest, tile_slot, parent_tiles, parent_blocks, sketch_test):
    test_blocks = sketch_test.reshape(PBLOCKS, TILE, SKETCH)
    sketch_acc = jnp.zeros((PBLOCKS, TILE, SKETCH), jnp.float32)
    results = []
    for child_id in range(N_CHILD):
        panel_blocks = panel[child_id].reshape(BLOCKS, TILE, TILE)
        basis_blocks = bases[child_id].reshape(BLOCKS, TILE, RANK)
        panel_proj = jnp.einsum("bxr,bxy->bry", basis_blocks.astype(jnp.float32), panel_blocks.astype(jnp.float32)).astype(jnp.bfloat16)
        targets = (tile_dest[child_id, :, 0] * PARENT_DEV + tile_slot[child_id]).astype(jnp.int32)

        def advance(summed, pieces):
            tile_block, row_id, col_id, target = pieces
            left_basis = basis_blocks[row_id]
            right_basis = basis_blocks[col_id]
            half = jnp.dot(left_basis.T, tile_block, preferred_element_type=jnp.float32).astype(jnp.bfloat16)
            encoded = jnp.dot(half, right_basis, preferred_element_type=jnp.float32)
            cross = jnp.dot(panel_proj[row_id], panel_proj[col_id].T, preferred_element_type=jnp.float32)
            core = (encoded - cross).astype(jnp.bfloat16)
            left_part = jnp.dot(left_basis, core, preferred_element_type=jnp.float32).astype(jnp.bfloat16)
            decoded = jnp.dot(left_part, right_basis.T, preferred_element_type=jnp.float32)
            return summed.at[target].add(decoded), None

        summed, _ = lax.scan(advance, parent_tiles[child_id].astype(jnp.float32),
                             (child_tiles[child_id], tile_blocks[child_id, :, 0], tile_blocks[child_id, :, 1], targets))
        updated = summed.astype(jnp.bfloat16)
        results.append(updated)

        def sketch_step(accum, pieces):
            parent_block, prow, pcol = pieces
            direct = jnp.dot(parent_block, test_blocks[pcol], preferred_element_type=jnp.float32)
            second = jnp.dot(parent_block.T, test_blocks[prow], preferred_element_type=jnp.float32)
            second = second * (prow != pcol).astype(jnp.float32)
            accum = accum.at[prow].add(direct)
            accum = accum.at[pcol].add(second)
            return accum, None

        sketch_acc, _ = lax.scan(sketch_step, sketch_acc, (updated, parent_blocks[child_id, :, 0], parent_blocks[child_id, :, 1]))
    return jnp.stack(results, axis=0), sketch_acc.reshape(PBLOCKS * TILE, SKETCH)
```

```python
import functools

import jax
import jax.numpy as jnp
from jax import lax
from jax.experimental import pallas as pl
from jax.experimental.pallas import tpu as pltpu
from jax.sharding import PartitionSpec as P

CAP = 2
LINE_OWNERS = 8
VMEM_BYTES = 60 * 1024 * 1024
F32 = jnp.float32
BF16 = jnp.bfloat16
NT = (((1,), (1,)), ((), ()))


def dot(x, y):
    return jnp.dot(x, y, preferred_element_type=F32)


def params():
    return pltpu.CompilerParams(
        dimension_semantics=("arbitrary",), vmem_limit_bytes=VMEM_BYTES
    )


def project_kernel(panel_ref, basis_ref, out_ref):
    rank = basis_ref.shape[2]
    flipped = basis_ref[0].T
    out_ref[0, :rank] = flipped
    out_ref[0, rank:] = dot(flipped, panel_ref[0]).astype(BF16)


def project(panel, bases, order):
    blocks = panel.shape[0] // order
    width, rank = panel.shape[1], bases.shape[1]
    return pl.pallas_call(
        project_kernel,
        grid=(blocks,),
        in_specs=[
            pl.BlockSpec((1, order, width), lambda b: (b, 0, 0)),
            pl.BlockSpec((1, order, rank), lambda b: (b, 0, 0)),
        ],
        out_specs=pl.BlockSpec((1, 2 * rank, order), lambda b: (b, 0, 0)),
        out_shape=jax.ShapeDtypeStruct((blocks, 2 * rank, order), BF16),
        compiler_params=params(),
        name="project",
    )(panel.reshape(blocks, order, width), bases.reshape(blocks, order, rank))


def along_chips(x, owners, shift):
    pairs = [(t, t + 2 * shift) for t in range(owners) if 0 <= t + 2 * shift < owners]
    return lax.ppermute(x, "tile", pairs)


def to_partner(x, owners):
    return lax.ppermute(x, "tile", [(t, t ^ 1) for t in range(owners)])


def spread(block, owners):
    if owners > LINE_OWNERS or owners % 2:
        return [lax.all_gather(block, "tile", axis=0, tiled=True)], None
    arrays, offsets = [block], [0]
    up, down = block, block
    for step in range(1, owners // 2):
        up, down = along_chips(up, owners, 1), along_chips(down, owners, -1)
        arrays += [up, down]
        offsets += [-step, step]
    return arrays + [to_partner(x, owners) for x in arrays], offsets


def encode_kernel(offsets, rows, cols, places, tile_ref, *refs):
    parts, (core_ref, flip_ref, held, sems, out_sem) = refs[:-5], refs[-5:]
    rank = core_ref.shape[1]
    step = pl.program_id(0)
    out_copy = pltpu.make_async_copy(held.at[:, :rank], flip_ref, out_sem)

    def each(act):
        if offsets is None:
            act(pltpu.make_async_copy(parts[0], held, sems.at[0]))
            return
        local = parts[0].shape[0]
        me = lax.axis_index("tile")
        chips = lax.axis_size("tile") // 2
        chip, core = me // 2, me % 2
        count = len(offsets)
        for n, part in enumerate(parts):
            source = chip + offsets[n % count]
            owner = source * 2 + (core if n < count else 1 - core)

            @pl.when((source >= 0) & (source < chips))
            def _():
                act(
                    pltpu.make_async_copy(
                        part, held.at[pl.ds(owner * local, local)], sems.at[n]
                    )
                )

    @pl.when(step == 0)
    def _():
        each(lambda copy: copy.start())
        if core_ref.shape[0] != pl.num_programs(0):
            core_ref[...] = jnp.zeros_like(core_ref)
        each(lambda copy: copy.wait())
        out_copy.start()

    row, col = rows[step], cols[step]
    half = dot(held[row, :rank], tile_ref[0]).astype(BF16)
    encoded = lax.dot_general(half, held[col, :rank], NT, preferred_element_type=F32)
    cross = lax.dot_general(
        held[row, rank:], held[col, rank:], NT, preferred_element_type=F32
    )
    core_ref[places[step]] = (encoded - cross).astype(BF16)

    @pl.when(step == pl.num_programs(0) - 1)
    def _():
        out_copy.wait()


def encode(tiles, parts, offsets, rows, cols, places, owners):
    count, order, _ = tiles.shape
    rank = parts[0].shape[1] // 2
    blocks = parts[0].shape[0] * (1 if offsets is None else owners)
    slots = owners * CAP
    return pl.pallas_call(
        functools.partial(encode_kernel, offsets),
        grid_spec=pltpu.PrefetchScalarGridSpec(
            num_scalar_prefetch=3,
            grid=(count,),
            in_specs=[pl.BlockSpec((1, order, order), lambda q, *_: (q, 0, 0))]
            + [pl.BlockSpec(memory_space=pl.ANY)] * len(parts),
            out_specs=[
                pl.BlockSpec((slots, rank, rank), lambda q, *_: (0, 0, 0)),
                pl.BlockSpec(memory_space=pl.ANY),
            ],
            scratch_shapes=[
                pltpu.VMEM((blocks, 2 * rank, order), BF16),
                pltpu.SemaphoreType.DMA((len(parts),)),
                pltpu.SemaphoreType.DMA,
            ],
        ),
        out_shape=[
            jax.ShapeDtypeStruct((slots, rank, rank), BF16),
            jax.ShapeDtypeStruct((blocks, rank, order), BF16),
        ],
        compiler_params=params(),
        name="encode",
    )(rows, cols, places, tiles, *parts)


def flip_kernel(x_ref, out_ref):
    out_ref[0] = x_ref[0].T


def flip(x, name):
    blocks, rows, cols = x.shape
    return pl.pallas_call(
        flip_kernel,
        grid=(blocks,),
        in_specs=[pl.BlockSpec((1, rows, cols), lambda b: (b, 0, 0))],
        out_specs=pl.BlockSpec((1, cols, rows), lambda b: (b, 0, 0)),
        out_shape=jax.ShapeDtypeStruct((blocks, cols, rows), x.dtype),
        compiler_params=params(),
        name=name,
    )(x)


def decode_kernel(
    rows, cols, slots, prows, pcols,
    parent_ref, core_ref, basis_ref, flip_ref, test_ref,
    updated_ref, keep_ref, send_ref, total, sketch,
):
    p = pl.program_id(0)
    rank = core_ref.shape[1]
    lanes = sketch.shape[2]
    pieces = parent_ref.shape[1] // lanes

    @pl.when(p == 0)
    def _():
        sketch[...] = jnp.zeros_like(sketch)

    total[...] = parent_ref[0].astype(F32)

    def item(s, carry):
        @pl.when(slots[s] == p)
        def _():
            left = dot(basis_ref[rows[s]], core_ref[s]).astype(BF16)
            total[...] += dot(left, flip_ref[cols[s]])

        return carry

    lax.fori_loop(0, core_ref.shape[0], item, 0)
    tile = total[...].astype(BF16)
    updated_ref[0] = tile
    prow, pcol = prows[p], pcols[p]

    def add(block, value):
        for r in range(pieces):
            sketch[block * pieces + r] += value[:, r * lanes : (r + 1) * lanes]

    add(prow, lax.dot_general(test_ref[pcol], tile, NT, preferred_element_type=F32))

    @pl.when(prow != pcol)
    def _():
        add(pcol, dot(test_ref[prow], tile))

    @pl.when(p == pl.num_programs(0) - 1)
    def _():
        core = lax.axis_index("tile") % 2
        for n in range(keep_ref.shape[0]):
            keep_ref[n] = sketch[2 * n + core].astype(BF16)
            send_ref[n] = sketch[2 * n + 1 - core].astype(BF16)


def decode(parents, cores, basis, flipped, test, rows, cols, slots, prows, pcols, lanes):
    count, order, _ = parents.shape
    width = test.shape[1]
    chunks = test.shape[0] * test.shape[2] // lanes

    def whole(x):
        return pl.BlockSpec(x.shape, lambda p, *_: (0, 0, 0))

    half = jax.ShapeDtypeStruct((chunks // 2, width, lanes), BF16)
    tile_spec = pl.BlockSpec((1, order, order), lambda p, *_: (p, 0, 0))
    return pl.pallas_call(
        decode_kernel,
        grid_spec=pltpu.PrefetchScalarGridSpec(
            num_scalar_prefetch=5,
            grid=(count,),
            in_specs=[tile_spec, whole(cores), whole(basis), whole(flipped), whole(test)],
            out_specs=[tile_spec, whole(half), whole(half)],
            scratch_shapes=[
                pltpu.VMEM((order, order), F32),
                pltpu.VMEM((chunks, width, lanes), F32),
            ],
        ),
        out_shape=[jax.ShapeDtypeStruct(parents.shape, BF16), half, half],
        compiler_params=params(),
        name="decode",
    )(rows, cols, slots, prows, pcols, parents, cores, basis, flipped, test)


def exchange_sum(pieces, axis, size, me, send, group):
    mine = lax.dynamic_slice_in_dim(pieces, me * group, group, 0)
    for shift in range(1, size):
        peer = (me + shift) % size
        out = lax.dynamic_slice_in_dim(pieces, peer * group, group, 0).astype(BF16)
        mine = mine + send(out, shift).astype(F32)
    return mine


def reduce_sketch(keep, sent, owners, children):
    child, tile = lax.axis_index("child"), lax.axis_index("tile")
    chips = owners // 2
    pieces = keep.astype(F32) + to_partner(sent, owners).astype(F32)

    def over_child(x, shift):
        return lax.ppermute(
            x, "child", [(i, (i + shift) % children) for i in range(children)]
        )

    def over_chips(x, shift):
        return lax.ppermute(
            x, "tile", [(t, (t + 2 * shift) % owners) for t in range(owners)]
        )

    pieces = exchange_sum(pieces, "child", children, child, over_child, chips)
    return exchange_sum(pieces, "tile", chips, tile // 2, over_chips, 1)[0]


def shards(
    child_tiles,
    panel,
    bases,
    tile_blocks,
    tile_dest,
    tile_slot,
    parent_tiles,
    parent_blocks,
    sketch_test,
):
    owners, children = lax.axis_size("tile"), lax.axis_size("child")
    myself = lax.axis_index("tile")
    tile_count, order = child_tiles.shape[1], child_tiles.shape[2]
    parent_count = parent_tiles.shape[1]

    block = project(panel[0], bases[0], order)
    parts, offsets = spread(block, owners)

    blocks_all = tile_blocks[0]
    own_blocks = lax.dynamic_slice_in_dim(blocks_all, myself * tile_count, tile_count, 0)
    dest_all = tile_dest[0, :, 0].reshape(owners, tile_count)
    own_dest = lax.dynamic_index_in_dim(dest_all, myself, 0, keepdims=False)
    ids = jnp.arange(tile_count, dtype=jnp.int32)
    before = (own_dest[:, None] == own_dest[None, :]) & (ids[None, :] < ids[:, None])
    places = own_dest * CAP + jnp.sum(before.astype(jnp.int32), axis=1)

    arrive = (dest_all == myself).astype(jnp.int32)
    earlier = jnp.sum(
        arrive[:, None, :] * (ids[None, None, :] < ids[None, :, None]).astype(jnp.int32), axis=2
    )
    turn = jnp.arange(CAP, dtype=jnp.int32)
    matched = arrive[:, None, :] * (earlier[:, None, :] == turn[None, :, None]).astype(jnp.int32)

    def received(values):
        return jnp.sum(matched * values.reshape(owners, 1, tile_count), axis=2).reshape(-1)

    live = jnp.sum(matched, axis=2).reshape(-1)
    recv_rows = received(blocks_all[:, 0])
    recv_cols = received(blocks_all[:, 1])
    recv_slots = jnp.where(live > 0, received(tile_slot[0]), parent_count)

    cores, flipped = encode(
        child_tiles[0], parts, offsets, own_blocks[:, 0], own_blocks[:, 1], places, owners
    )
    rank = cores.shape[1]
    incoming = lax.all_to_all(
        cores.reshape(owners, CAP, rank, rank), "tile", split_axis=0, concat_axis=0, tiled=True
    ).reshape(cores.shape)
    basis = flip(flipped, "flip_basis")
    width = sketch_test.shape[1]
    test = flip(sketch_test.reshape(-1, order, width), "flip_test")
    lanes = sketch_test.shape[0] // (owners * children)
    updated, keep, sent = decode(
        parent_tiles[0], incoming, basis, flipped, test,
        recv_rows, recv_cols, recv_slots,
        parent_blocks[0, :, 0], parent_blocks[0, :, 1], lanes,
    )
    sketch = reduce_sketch(keep, sent, owners, children)
    return updated[None], sketch.T


def solution(mesh):
    return jax.shard_map(
        shards,
        mesh=mesh,
        in_specs=(
            P("child", "tile", None, None),
            P("child", "tile", None),
            P("child", "tile", None),
            P("child", None, None),
            P("child", None, None),
            P("child", None),
            P("child", "tile", None, None),
            P("child", "tile", None),
            P(),
        ),
        out_specs=(P("child", "tile", None, None), P(("child", "tile"), None)),
        check_vma=False,
    )
```

```python
import jax
import jax.numpy as jnp
from jax import lax
from jax.experimental import pallas as pl
from jax.experimental.pallas import tpu as pltpu
from jax.sharding import PartitionSpec as P

CAP = 2
RING_OWNERS = 8
VMEM_BYTES = 58 * 1024 * 1024
F32 = jnp.float32
BF16 = jnp.bfloat16
NT = (((1,), (1,)), ((), ()))


def dot(x, y):
    return jnp.dot(x, y, preferred_element_type=F32)


def params():
    return pltpu.CompilerParams(vmem_limit_bytes=VMEM_BYTES)


def project_kernel(panel_ref, basis_ref, out_ref):
    rank = basis_ref.shape[2]
    flipped = basis_ref[0].T
    out_ref[0, :rank] = flipped
    out_ref[0, rank:] = dot(flipped, panel_ref[0]).astype(BF16)


def project(panel, bases, order):
    blocks = panel.shape[0] // order
    width, rank = panel.shape[1], bases.shape[1]
    return pl.pallas_call(
        project_kernel,
        grid=(blocks,),
        in_specs=[
            pl.BlockSpec((1, order, width), lambda b: (b, 0, 0)),
            pl.BlockSpec((1, order, rank), lambda b: (b, 0, 0)),
        ],
        out_specs=pl.BlockSpec((1, 2 * rank, order), lambda b: (b, 0, 0)),
        out_shape=jax.ShapeDtypeStruct((blocks, 2 * rank, order), BF16),
        compiler_params=params(),
        name="project",
    )(panel.reshape(blocks, order, width), bases.reshape(blocks, order, rank))


def along_chips(x, owners, shift):
    return lax.ppermute(x, "tile", [(t, (t + 2 * shift) % owners) for t in range(owners)])


def to_partner(x, owners):
    return lax.ppermute(x, "tile", [(t, t ^ 1) for t in range(owners)])


def spread(block, owners):
    if owners > RING_OWNERS or owners % 4:
        return [lax.all_gather(block, "tile", axis=0, tiled=True)], None
    far, half = owners // 4, block.shape[1] // 2
    arrays, places = [block], [(0, 0)]
    up, down = block, block
    for step in range(1, far + 1):
        if step == far:
            up, down = up[:, :half], down[:, half:]
        up, down = along_chips(up, owners, 1), along_chips(down, owners, -1)
        arrays += [up, down]
        places += [(-step, 0), (step, half if step == far else 0)]
    return arrays + [to_partner(x, owners) for x in arrays], places


def unpack(word, blocks):
    rest = word // blocks
    return rest // blocks, rest % blocks, word % blocks


SCALARS = pl.BlockSpec(memory_space=pltpu.SMEM)
ANYWHERE = pl.BlockSpec(memory_space=pl.ANY)
IN_HBM = pl.BlockSpec(memory_space=pltpu.HBM)
ON_CHIP = pl.BlockSpec(memory_space=pltpu.VMEM)


def encode_kernel(places, count, words, tiles, *refs):
    parts = refs[:-10]
    core_out, flip_out = refs[-10:-8]
    held, staged, coded, tile_sems, part_sems, core_sems, flip_sem = refs[-8:-1]
    blocks = held.shape[0]
    rank = core_out.shape[1]
    flip_copy = pltpu.make_async_copy(held.at[:, :rank], flip_out, flip_sem)

    def part_copies():
        if places is None:
            return [pltpu.make_async_copy(parts[0], held, part_sems.at[0])]
        local = parts[0].shape[0]
        me = lax.axis_index("tile")
        chips = lax.axis_size("tile") // 2
        chip, core = me // 2, me % 2
        copies = []
        for n, part in enumerate(parts):
            offset, first = places[n % len(places)]
            owner = ((chip + chips + offset) % chips) * 2
            owner = owner + (core if n < len(places) else 1 - core)
            copies.append(
                pltpu.make_async_copy(
                    part,
                    held.at[pl.ds(owner * local, local), pl.ds(first, part.shape[1])],
                    part_sems.at[n],
                )
            )
        return copies

    def tile_copy(q):
        return pltpu.make_async_copy(tiles.at[q], staged.at[q], tile_sems.at[q])

    def core_copy(q, place):
        return pltpu.make_async_copy(coded.at[q], core_out.at[place], core_sems.at[q])

    copies = part_copies()
    for copy in copies:
        copy.start()
    for q in range(count):
        tile_copy(q).start()
    for copy in copies:
        copy.wait()
    flip_copy.start()

    def one(q, carry):
        place, row, col = unpack(words[q], blocks)
        tile_copy(q).wait()
        half = dot(held[row, :rank], staged[q]).astype(BF16)
        encoded = lax.dot_general(half, held[col, :rank], NT, preferred_element_type=F32)
        cross = lax.dot_general(
            held[row, rank:], held[col, rank:], NT, preferred_element_type=F32
        )
        coded[q] = (encoded - cross).astype(BF16)
        core_copy(q, place).start()
        return carry

    lax.fori_loop(0, count, one, 0, unroll=4)
    for q in range(count):
        core_copy(q, 0).wait()
    flip_copy.wait()


def encode(tiles, parts, places, words, owners):
    count, order, _ = tiles.shape
    rank = parts[0].shape[1] // 2
    blocks = parts[0].shape[0] * (1 if places is None else owners)
    slots = owners * CAP

    def body(words, tiles, *refs):
        encode_kernel(places, count, words, tiles, *refs, None)

    return pl.pallas_call(
        body,
        in_specs=[SCALARS, IN_HBM] + [ANYWHERE] * len(parts),
        out_specs=[ANYWHERE, ANYWHERE],
        scratch_shapes=[
            pltpu.VMEM((blocks, 2 * rank, order), BF16),
            pltpu.VMEM(tiles.shape, BF16),
            pltpu.VMEM((count, rank, rank), BF16),
            pltpu.SemaphoreType.DMA((count,)),
            pltpu.SemaphoreType.DMA((len(parts),)),
            pltpu.SemaphoreType.DMA((count,)),
            pltpu.SemaphoreType.DMA,
        ],
        out_shape=[
            jax.ShapeDtypeStruct((slots, rank, rank), BF16),
            jax.ShapeDtypeStruct((blocks, rank, order), BF16),
        ],
        compiler_params=params(),
        name="encode",
    )(words, tiles, *parts)


def add_rows(sketch, block, value):
    lanes = sketch.shape[2]
    pieces = value.shape[1] // lanes
    for r in range(pieces):
        sketch[block * pieces + r] += value[:, r * lanes : (r + 1) * lanes]


def prepare_kernel(words, pwords, flip_ref, test_ref, parents, basis_ref, west, vest, sketch, turned):
    blocks, tests = flip_ref.shape[0], test_ref.shape[0]
    count = parents.shape[0]
    sketch[...] = jnp.zeros_like(sketch)
    for b in range(tests):
        turned[b] = test_ref[b].T
    for b in range(blocks):
        basis_ref[b] = flip_ref[b].T

    def parent(p, carry):
        prow, pcol = pwords[2 * p], pwords[2 * p + 1]
        add_rows(
            sketch,
            prow,
            lax.dot_general(turned[pcol], parents[p], NT, preferred_element_type=F32),
        )

        @pl.when(prow != pcol)
        def _():
            add_rows(sketch, pcol, dot(turned[prow], parents[p]))

        return carry

    lax.fori_loop(0, count, parent, 0)

    def item(s, carry):
        slot, row, col = unpack(words[s], blocks)

        @pl.when(slot > 0)
        def _():
            prow, pcol = pwords[2 * slot - 2], pwords[2 * slot - 1]
            west[s] = lax.dot_general(
                turned[pcol], flip_ref[col], NT, preferred_element_type=F32
            ).astype(BF16)
            vest[s] = lax.dot_general(
                turned[prow], flip_ref[row], NT, preferred_element_type=F32
            ).astype(BF16)

        return carry

    lax.fori_loop(0, west.shape[0], item, 0)


def prepare(words, pwords, flipped, test, parents, lanes):
    blocks, rank, order = flipped.shape
    tests, _, width = test.shape
    items = words.shape[0]
    return pl.pallas_call(
        prepare_kernel,
        in_specs=[SCALARS, SCALARS, ON_CHIP, ON_CHIP, ON_CHIP],
        out_specs=[ON_CHIP] * 4,
        scratch_shapes=[pltpu.VMEM((tests, width, order), BF16)],
        out_shape=[
            jax.ShapeDtypeStruct((blocks, order, rank), BF16),
            jax.ShapeDtypeStruct((items, width, rank), BF16),
            jax.ShapeDtypeStruct((items, width, rank), BF16),
            jax.ShapeDtypeStruct((tests * order // lanes, width, lanes), F32),
        ],
        compiler_params=params(),
        cost_estimate=pl.CostEstimate(
            flops=4 * parents.size * width, bytes_accessed=2 * parents.size, transcendentals=0
        ),
        name="prepare",
    )(words, pwords, flipped, test, parents)


def fold_kernel(
    words, pwords, core_ref, west, vest, flip_ref, start, keep_ref, send_ref, sketch, base, sem
):
    blocks = flip_ref.shape[0]
    base_copy = pltpu.make_async_copy(start, base, sem)
    base_copy.start()
    sketch[...] = jnp.zeros_like(sketch)

    def item(s, carry):
        slot, row, col = unpack(words[s], blocks)

        @pl.when(slot > 0)
        def _():
            prow, pcol = pwords[2 * slot - 2], pwords[2 * slot - 1]
            first = lax.dot_general(west[s], core_ref[s], NT, preferred_element_type=F32)
            add_rows(sketch, prow, dot(first.astype(BF16), flip_ref[row]))

            @pl.when(prow != pcol)
            def _():
                second = dot(vest[s], core_ref[s]).astype(BF16)
                add_rows(sketch, pcol, dot(second, flip_ref[col]))

        return carry

    lax.fori_loop(0, core_ref.shape[0], item, 0)
    base_copy.wait()
    core = lax.axis_index("tile") % 2
    for n in range(keep_ref.shape[0]):
        mine, other = 2 * n + core, 2 * n + 1 - core
        keep_ref[n] = (sketch[mine] + base[mine]).astype(BF16)
        send_ref[n] = (sketch[other] + base[other]).astype(BF16)


def fold(words, pwords, cores, west, vest, flipped, start):
    chunks, width, lanes = start.shape
    half = jax.ShapeDtypeStruct((chunks // 2, width, lanes), BF16)
    return pl.pallas_call(
        fold_kernel,
        in_specs=[SCALARS, SCALARS] + [ON_CHIP] * 4 + [ANYWHERE],
        out_specs=[ON_CHIP, ON_CHIP],
        scratch_shapes=[
            pltpu.VMEM(start.shape, F32),
            pltpu.VMEM(start.shape, F32),
            pltpu.SemaphoreType.DMA,
        ],
        out_shape=[half, half],
        compiler_params=params(),
        name="fold",
    )(words, pwords, cores, west, vest, flipped, start)


def update_kernel(
    words, parents, core_ref, basis_ref, flip_ref, updated, held, total, made, in_sems, out_sems
):
    count, blocks = held.shape[0], basis_ref.shape[0]

    def in_copy(p):
        return pltpu.make_async_copy(parents.at[p], held.at[p], in_sems.at[p])

    def out_copy(p):
        return pltpu.make_async_copy(made.at[p], updated.at[p], out_sems.at[p])

    for p in range(count):
        in_copy(p).start()

    def one(p, carry):
        in_copy(p).wait()
        total[...] = held[p].astype(F32)

        def item(s, carry):
            slot, row, col = unpack(words[s], blocks)

            @pl.when(slot == p + 1)
            def _():
                left = dot(basis_ref[row], core_ref[s]).astype(BF16)
                total[...] += dot(left, flip_ref[col])

            return carry

        lax.fori_loop(0, core_ref.shape[0], item, 0)
        made[p] = total[...].astype(BF16)
        out_copy(p).start()
        return carry

    lax.fori_loop(0, count, one, 0)
    for p in range(count):
        out_copy(p).wait()


def update(words, parents, cores, basis, flipped):
    count, order, _ = parents.shape
    rank = basis.shape[2]
    return pl.pallas_call(
        update_kernel,
        in_specs=[SCALARS, IN_HBM, ON_CHIP, ON_CHIP, ON_CHIP],
        out_specs=IN_HBM,
        scratch_shapes=[
            pltpu.VMEM(parents.shape, BF16),
            pltpu.VMEM((order, order), F32),
            pltpu.VMEM(parents.shape, BF16),
            pltpu.SemaphoreType.DMA((count,)),
            pltpu.SemaphoreType.DMA((count,)),
        ],
        out_shape=jax.ShapeDtypeStruct(parents.shape, BF16),
        compiler_params=params(),
        cost_estimate=pl.CostEstimate(
            flops=8 * parents.size * rank, bytes_accessed=4 * parents.size, transcendentals=0
        ),
        name="update",
    )(words, parents, cores, basis, flipped)


def exchange_sum(pieces, size, me, send, group):
    mine = lax.dynamic_slice_in_dim(pieces, me * group, group, 0)
    for shift in range(1, size):
        peer = (me + shift) % size
        out = lax.dynamic_slice_in_dim(pieces, peer * group, group, 0).astype(BF16)
        mine = mine + send(out, shift).astype(F32)
    return mine


def reduce_sketch(keep, sent, updated, owners, children):
    child, tile = lax.axis_index("child"), lax.axis_index("tile")
    chips = owners // 2
    pieces = keep.astype(F32) + to_partner(sent, owners).astype(F32)

    def over_child(x, shift):
        return lax.ppermute(
            x, "child", [(i, (i + shift) % children) for i in range(children)]
        )

    def over_chips(x, shift):
        return lax.ppermute(
            x, "tile", [(t, (t + 2 * shift) % owners) for t in range(owners)]
        )

    pieces = exchange_sum(pieces, children, child, over_child, chips)
    pieces, updated = lax.optimization_barrier((pieces, updated))
    return exchange_sum(pieces, chips, tile // 2, over_chips, 1)[0], updated


def shards(
    child_tiles,
    panel,
    bases,
    tile_blocks,
    tile_dest,
    tile_slot,
    parent_tiles,
    parent_blocks,
    sketch_test,
):
    owners, children = lax.axis_size("tile"), lax.axis_size("child")
    myself = lax.axis_index("tile")
    tile_count, order = child_tiles.shape[1], child_tiles.shape[2]

    block = project(panel[0], bases[0], order)
    parts, places = spread(block, owners)

    blocks = owners * panel.shape[1] // order
    pair_all = (tile_blocks[0, :, 0] * blocks + tile_blocks[0, :, 1]).reshape(owners, tile_count)
    dest_all = tile_dest[0, :, 0].reshape(owners, tile_count)
    own_pair = lax.dynamic_index_in_dim(pair_all, myself, 0, keepdims=False)
    own_dest = lax.dynamic_index_in_dim(dest_all, myself, 0, keepdims=False)
    ids = jnp.arange(tile_count, dtype=jnp.int32)
    lower = ids[None, :] < ids[:, None]
    before = (own_dest[:, None] == own_dest[None, :]) & lower
    place = own_dest * CAP + jnp.sum(before.astype(jnp.int32), axis=1)
    own_words = place * (blocks * blocks) + own_pair

    arrive = dest_all == myself
    earlier = jnp.sum((arrive[:, None, :] & lower[None]).astype(jnp.int32), axis=2)
    turn = jnp.arange(CAP, dtype=jnp.int32)
    matched = arrive[:, None, :] & (earlier[:, None, :] == turn[None, :, None])
    word_all = (tile_slot[0].reshape(owners, tile_count) + 1) * (blocks * blocks) + pair_all
    words = jnp.sum(jnp.where(matched, word_all[:, None, :], 0), axis=2).reshape(-1)
    pwords = parent_blocks[0].reshape(-1)

    cores, flipped = encode(child_tiles[0], parts, places, own_words, owners)
    rank = cores.shape[1]
    incoming = lax.all_to_all(
        cores.reshape(owners, CAP, rank, rank), "tile", split_axis=0, concat_axis=0, tiled=True
    ).reshape(cores.shape)
    width = sketch_test.shape[1]
    lanes = sketch_test.shape[0] // (owners * children)
    basis, west, vest, start = prepare(
        words, pwords, flipped, sketch_test.reshape(-1, order, width), parent_tiles[0], lanes
    )
    keep, sent = fold(words, pwords, incoming, west, vest, flipped, start)
    updated = update(words, parent_tiles[0], incoming, basis, flipped)
    sketch, updated = reduce_sketch(keep, sent, updated, owners, children)
    return updated[None], sketch.T


def solution(mesh):
    return jax.shard_map(
        shards,
        mesh=mesh,
        in_specs=(
            P("child", "tile", None, None),
            P("child", "tile", None),
            P("child", "tile", None),
            P("child", None, None),
            P("child", None, None),
            P("child", None),
            P("child", "tile", None, None),
            P("child", "tile", None),
            P(),
        ),
        out_specs=(P("child", "tile", None, None), P(("child", "tile"), None)),
        check_vma=False,
    )
```

```python
import jax
import jax.numpy as jnp
from jax import lax
from jax.experimental import pallas as pl
from jax.experimental.pallas import tpu as pltpu
from jax.sharding import PartitionSpec as P

CAP = 2
RING_OWNERS = 8
VMEM_BYTES = 58 * 1024 * 1024
F32 = jnp.float32
BF16 = jnp.bfloat16
NT = (((1,), (1,)), ((), ()))


def dot(x, y):
    return jnp.dot(x, y, preferred_element_type=F32)


def params():
    return pltpu.CompilerParams(vmem_limit_bytes=VMEM_BYTES)


def project_kernel(panel_ref, basis_ref, out_ref):
    rank = basis_ref.shape[2]
    flipped = basis_ref[0].T
    out_ref[0, :rank] = flipped
    out_ref[0, rank:] = dot(flipped, panel_ref[0]).astype(BF16)


def project(panel, bases, order):
    blocks = panel.shape[0] // order
    width, rank = panel.shape[1], bases.shape[1]
    return pl.pallas_call(
        project_kernel,
        grid=(blocks,),
        in_specs=[
            pl.BlockSpec((1, order, width), lambda b: (b, 0, 0)),
            pl.BlockSpec((1, order, rank), lambda b: (b, 0, 0)),
        ],
        out_specs=pl.BlockSpec((1, 2 * rank, order), lambda b: (b, 0, 0)),
        out_shape=jax.ShapeDtypeStruct((blocks, 2 * rank, order), BF16),
        compiler_params=params(),
        name="project",
    )(panel.reshape(blocks, order, width), bases.reshape(blocks, order, rank))


def along_chips(x, owners, shift):
    return lax.ppermute(x, "tile", [(t, (t + 2 * shift) % owners) for t in range(owners)])


def to_partner(x, owners):
    return lax.ppermute(x, "tile", [(t, t ^ 1) for t in range(owners)])


def spread(block, owners):
    if owners > RING_OWNERS or owners % 4:
        return [lax.all_gather(block, "tile", axis=0, tiled=True)], None
    far, half = owners // 4, block.shape[1] // 2
    arrays, places = [block], [(0, 0)]
    up, down = block, block
    for step in range(1, far + 1):
        if step == far:
            up, down = up[:, :half], down[:, half:]
        up, down = along_chips(up, owners, 1), along_chips(down, owners, -1)
        arrays += [up, down]
        places += [(-step, 0), (step, half if step == far else 0)]
    return arrays + [to_partner(x, owners) for x in arrays], places


def grouped(count):
    return 4 if count % 4 == 0 else 1


def unpack(word, blocks):
    rest = word // blocks
    return rest // blocks, rest % blocks, word % blocks


SCALARS = pl.BlockSpec(memory_space=pltpu.SMEM)
ANYWHERE = pl.BlockSpec(memory_space=pl.ANY)
IN_HBM = pl.BlockSpec(memory_space=pltpu.HBM)
ON_CHIP = pl.BlockSpec(memory_space=pltpu.VMEM)


def encode_kernel(places, count, words, tiles, *refs):
    parts = refs[:-11]
    core_out, flip_out = refs[-11:-9]
    held, staged, crossed, tile_sems, part_sems, core_sems, flip_sem = refs[-9:-2]
    coded = refs[-2]
    blocks = held.shape[0]
    rank = core_out.shape[1]
    flip_copy = pltpu.make_async_copy(held.at[:, :rank], flip_out, flip_sem)

    def part_copies():
        if places is None:
            return [pltpu.make_async_copy(parts[0], held, part_sems.at[0])]
        local = parts[0].shape[0]
        me = lax.axis_index("tile")
        chips = lax.axis_size("tile") // 2
        chip, core = me // 2, me % 2
        copies = []
        for n, part in enumerate(parts):
            offset, first = places[n % len(places)]
            owner = ((chip + chips + offset) % chips) * 2
            owner = owner + (core if n < len(places) else 1 - core)
            copies.append(
                pltpu.make_async_copy(
                    part,
                    held.at[pl.ds(owner * local, local), pl.ds(first, part.shape[1])],
                    part_sems.at[n],
                )
            )
        return copies

    def tile_copy(q):
        return pltpu.make_async_copy(tiles.at[q], staged.at[q], tile_sems.at[q])

    def core_copy(q, place):
        return pltpu.make_async_copy(coded.at[q], core_out.at[place], core_sems.at[q])

    copies = part_copies()
    for copy in copies:
        copy.start()
    for q in range(count):
        tile_copy(q).start()
    for copy in copies:
        copy.wait()
    flip_copy.start()

    group = grouped(count)

    def cross(g, carry):
        for q in [g * group + n for n in range(group)]:
            _, row, col = unpack(words[q], blocks)
            crossed[q] = lax.dot_general(
                held[row, rank:], held[col, rank:], NT, preferred_element_type=F32
            )
        return carry

    def one(g, carry):
        tiles_now = [g * group + n for n in range(group)]
        keys = [unpack(words[q], blocks) for q in tiles_now]
        for q in tiles_now:
            tile_copy(q).wait()
        halves = [
            dot(held[row, :rank], staged[q]).astype(BF16)
            for q, (_, row, _) in zip(tiles_now, keys)
        ]
        cores = [
            lax.dot_general(half, held[col, :rank], NT, preferred_element_type=F32)
            for half, (_, _, col) in zip(halves, keys)
        ]
        for q, core in zip(tiles_now, cores):
            coded[q] = (core - crossed[q]).astype(BF16)
        for q, (place, _, _) in zip(tiles_now, keys):
            core_copy(q, place).start()
        return carry

    lax.fori_loop(0, count // group, cross, 0)
    lax.fori_loop(0, count // group, one, 0)
    for q in range(count):
        core_copy(q, 0).wait()
    flip_copy.wait()


def encode(tiles, parts, places, words, owners):
    count, order, _ = tiles.shape
    rank = parts[0].shape[1] // 2
    blocks = parts[0].shape[0] * (1 if places is None else owners)
    slots = owners * CAP

    def body(words, tiles, *refs):
        encode_kernel(places, count, words, tiles, *refs, None)

    return pl.pallas_call(
        body,
        in_specs=[SCALARS, IN_HBM] + [ANYWHERE] * len(parts),
        out_specs=[ANYWHERE, ANYWHERE],
        scratch_shapes=[
            pltpu.VMEM((blocks, 2 * rank, order), BF16),
            pltpu.VMEM(tiles.shape, BF16),
            pltpu.VMEM((count, rank, rank), F32),
            pltpu.SemaphoreType.DMA((count,)),
            pltpu.SemaphoreType.DMA((len(parts),)),
            pltpu.SemaphoreType.DMA((count,)),
            pltpu.SemaphoreType.DMA,
            pltpu.VMEM((count, rank, rank), BF16),
        ],
        out_shape=[
            jax.ShapeDtypeStruct((slots, rank, rank), BF16),
            jax.ShapeDtypeStruct((blocks, rank, order), BF16),
        ],
        compiler_params=params(),
        name="encode",
    )(words, tiles, *parts)


def add_rows(sketch, block, value):
    lanes = sketch.shape[2]
    pieces = value.shape[1] // lanes
    for r in range(pieces):
        sketch[block * pieces + r] += value[:, r * lanes : (r + 1) * lanes]


def prepare_kernel(words, pwords, flip_ref, test_ref, parents, basis_ref, west, vest, sketch, turned):
    blocks, tests = flip_ref.shape[0], test_ref.shape[0]
    count = parents.shape[0]
    sketch[...] = jnp.zeros_like(sketch)
    for b in range(tests):
        turned[b] = test_ref[b].T
    for b in range(blocks):
        basis_ref[b] = flip_ref[b].T

    def parent(p, carry):
        prow, pcol = pwords[2 * p], pwords[2 * p + 1]
        add_rows(
            sketch,
            prow,
            lax.dot_general(turned[pcol], parents[p], NT, preferred_element_type=F32),
        )

        @pl.when(prow != pcol)
        def _():
            add_rows(sketch, pcol, dot(turned[prow], parents[p]))

        return carry

    lax.fori_loop(0, count, parent, 0)

    group = grouped(west.shape[0])

    def item(g, carry):
        for s in [g * group + n for n in range(group)]:
            slot, row, col = unpack(words[s], blocks)
            at = 2 * jnp.maximum(slot - 1, 0)
            west[s] = lax.dot_general(
                turned[pwords[at + 1]], flip_ref[col], NT, preferred_element_type=F32
            ).astype(BF16)
            vest[s] = lax.dot_general(
                turned[pwords[at]], flip_ref[row], NT, preferred_element_type=F32
            ).astype(BF16)
        return carry

    lax.fori_loop(0, west.shape[0] // group, item, 0)


def prepare(words, pwords, flipped, test, parents, lanes):
    blocks, rank, order = flipped.shape
    tests, _, width = test.shape
    items = words.shape[0]
    return pl.pallas_call(
        prepare_kernel,
        in_specs=[SCALARS, SCALARS, ON_CHIP, ON_CHIP, ON_CHIP],
        out_specs=[ON_CHIP] * 4,
        scratch_shapes=[pltpu.VMEM((tests, width, order), BF16)],
        out_shape=[
            jax.ShapeDtypeStruct((blocks, order, rank), BF16),
            jax.ShapeDtypeStruct((items, width, rank), BF16),
            jax.ShapeDtypeStruct((items, width, rank), BF16),
            jax.ShapeDtypeStruct((tests * order // lanes, width, lanes), F32),
        ],
        compiler_params=params(),
        cost_estimate=pl.CostEstimate(
            flops=4 * parents.size * width, bytes_accessed=2 * parents.size, transcendentals=0
        ),
        name="prepare",
    )(words, pwords, flipped, test, parents)


def fold_kernel(
    words, pwords, core_ref, west, vest, flip_ref, start, keep_ref, send_ref, sketch, base, sem
):
    blocks = flip_ref.shape[0]
    base_copy = pltpu.make_async_copy(start, base, sem)
    base_copy.start()
    sketch[...] = jnp.zeros_like(sketch)

    group = grouped(core_ref.shape[0])

    def item(g, carry):
        targets, values = [], []
        for s in [g * group + n for n in range(group)]:
            slot, row, col = unpack(words[s], blocks)
            at = 2 * jnp.maximum(slot - 1, 0)
            prow, pcol = pwords[at], pwords[at + 1]
            core = jnp.where(slot > 0, core_ref[s], jnp.zeros_like(core_ref[s]))
            first = lax.dot_general(west[s], core, NT, preferred_element_type=F32)
            second = jnp.where(prow != pcol, dot(vest[s], core), 0.0)
            targets += [prow, pcol]
            values += [(first.astype(BF16), row), (second.astype(BF16), col)]
        values = [dot(value, flip_ref[block]) for value, block in values]
        for target, value in zip(targets, values):
            add_rows(sketch, target, value)
        return carry

    lax.fori_loop(0, core_ref.shape[0] // group, item, 0)
    base_copy.wait()
    core = lax.axis_index("tile") % 2
    for n in range(keep_ref.shape[0]):
        mine, other = 2 * n + core, 2 * n + 1 - core
        keep_ref[n] = (sketch[mine] + base[mine]).astype(BF16)
        send_ref[n] = (sketch[other] + base[other]).astype(BF16)


def fold(words, pwords, cores, west, vest, flipped, start):
    chunks, width, lanes = start.shape
    half = jax.ShapeDtypeStruct((chunks // 2, width, lanes), BF16)
    return pl.pallas_call(
        fold_kernel,
        in_specs=[SCALARS, SCALARS] + [ON_CHIP] * 4 + [ANYWHERE],
        out_specs=[ON_CHIP, ON_CHIP],
        scratch_shapes=[
            pltpu.VMEM(start.shape, F32),
            pltpu.VMEM(start.shape, F32),
            pltpu.SemaphoreType.DMA,
        ],
        out_shape=[half, half],
        compiler_params=params(),
        name="fold",
    )(words, pwords, cores, west, vest, flipped, start)


def update_kernel(
    low, words, parents, partial, core_ref, basis_ref, flip_ref, updated,
    held, total, mixed, made, in_sems, out_sems,
):
    count, blocks, items = held.shape[0], basis_ref.shape[0], core_ref.shape[0]
    group = grouped(items)

    def in_copy(p):
        return pltpu.make_async_copy(parents.at[low + p], held.at[p], in_sems.at[p])

    def out_copy(p):
        return pltpu.make_async_copy(made.at[p], updated.at[low + p], out_sems.at[p])

    for p in range(count):
        in_copy(p).start()

    def mix(g, carry):
        for s in [g * group + n for n in range(group)]:
            _, _, col = unpack(words[s], blocks)
            mixed[s] = dot(core_ref[s], flip_ref[col]).astype(BF16)
        return carry

    lax.fori_loop(0, items // group, mix, 0)
    for p in range(count):
        in_copy(p).wait()
        total[p] = held[p].astype(F32)

    def item(s, carry):
        slot, row, _ = unpack(words[s], blocks)

        @pl.when((slot > low) & (slot <= low + count))
        def _():
            total[slot - 1 - low] += dot(basis_ref[row], mixed[s])

        return carry

    lax.fori_loop(0, items, item, 0)
    for p in range(count):
        made[p] = total[p].astype(BF16)
        out_copy(p).start()
    for p in range(count):
        out_copy(p).wait()


def update(low, count, words, parents, partial, cores, basis, flipped):
    order = parents.shape[1]
    rank = basis.shape[2]
    items = cores.shape[0]
    first = partial is None
    given = [] if first else [partial]

    def body(words, parents, *refs):
        update_kernel(low, words, parents, *([None] if first else []), *refs)

    return pl.pallas_call(
        body,
        in_specs=[SCALARS, IN_HBM] + [IN_HBM] * len(given) + [ON_CHIP] * 3,
        out_specs=IN_HBM,
        scratch_shapes=[
            pltpu.VMEM((count, order, order), BF16),
            pltpu.VMEM((count, order, order), F32),
            pltpu.VMEM((items, rank, order), BF16),
            pltpu.VMEM((count, order, order), BF16),
            pltpu.SemaphoreType.DMA((count,)),
            pltpu.SemaphoreType.DMA((count,)),
        ],
        out_shape=jax.ShapeDtypeStruct(parents.shape, BF16),
        input_output_aliases={} if first else {2: 0},
        compiler_params=params(),
        cost_estimate=pl.CostEstimate(
            flops=8 * parents.size * rank, bytes_accessed=4 * parents.size, transcendentals=0
        ),
        name="update",
    )(words, parents, *given, cores, basis, flipped)


def exchange_sum(pieces, size, me, send, group):
    mine = lax.dynamic_slice_in_dim(pieces, me * group, group, 0)
    for shift in range(1, size):
        peer = (me + shift) % size
        out = lax.dynamic_slice_in_dim(pieces, peer * group, group, 0).astype(BF16)
        mine = mine + send(out, shift).astype(F32)
    return mine


def reduce_sketch(keep, sent, decode, cores, owners, children):
    child, tile = lax.axis_index("child"), lax.axis_index("tile")
    chips = owners // 2
    pieces = keep.astype(F32) + to_partner(sent, owners).astype(F32)

    def over_child(x, shift):
        return lax.ppermute(
            x, "child", [(i, (i + shift) % children) for i in range(children)]
        )

    def over_chips(x, shift):
        return lax.ppermute(
            x, "tile", [(t, (t + 2 * shift) % owners) for t in range(owners)]
        )

    pieces = exchange_sum(pieces, children, child, over_child, chips)
    pieces, updated, cores = lax.optimization_barrier((pieces, decode(None, cores), cores))
    return exchange_sum(pieces, chips, tile // 2, over_chips, 1)[0], decode(updated, cores)


def shards(
    child_tiles,
    panel,
    bases,
    tile_blocks,
    tile_dest,
    tile_slot,
    parent_tiles,
    parent_blocks,
    sketch_test,
):
    owners, children = lax.axis_size("tile"), lax.axis_size("child")
    myself = lax.axis_index("tile")
    tile_count, order = child_tiles.shape[1], child_tiles.shape[2]

    block = project(panel[0], bases[0], order)
    parts, places = spread(block, owners)

    blocks = owners * panel.shape[1] // order
    pair_all = (tile_blocks[0, :, 0] * blocks + tile_blocks[0, :, 1]).reshape(owners, tile_count)
    dest_all = tile_dest[0, :, 0].reshape(owners, tile_count)
    own_pair = lax.dynamic_index_in_dim(pair_all, myself, 0, keepdims=False)
    own_dest = lax.dynamic_index_in_dim(dest_all, myself, 0, keepdims=False)
    ids = jnp.arange(tile_count, dtype=jnp.int32)
    lower = ids[None, :] < ids[:, None]
    before = (own_dest[:, None] == own_dest[None, :]) & lower
    place = own_dest * CAP + jnp.sum(before.astype(jnp.int32), axis=1)
    own_words = place * (blocks * blocks) + own_pair

    arrive = dest_all == myself
    earlier = jnp.sum((arrive[:, None, :] & lower[None]).astype(jnp.int32), axis=2)
    turn = jnp.arange(CAP, dtype=jnp.int32)
    matched = arrive[:, None, :] & (earlier[:, None, :] == turn[None, :, None])
    word_all = (tile_slot[0].reshape(owners, tile_count) + 1) * (blocks * blocks) + pair_all
    words = jnp.sum(jnp.where(matched, word_all[:, None, :], 0), axis=2).reshape(-1)
    pwords = parent_blocks[0].reshape(-1)

    cores, flipped = encode(child_tiles[0], parts, places, own_words, owners)
    rank = cores.shape[1]
    incoming = lax.all_to_all(
        cores.reshape(owners, CAP, rank, rank), "tile", split_axis=0, concat_axis=0, tiled=True
    ).reshape(cores.shape)
    width = sketch_test.shape[1]
    lanes = sketch_test.shape[0] // (owners * children)
    basis, west, vest, start = prepare(
        words, pwords, flipped, sketch_test.reshape(-1, order, width), parent_tiles[0], lanes
    )
    keep, sent = fold(words, pwords, incoming, west, vest, flipped, start)

    def decode(partial, cores):
        count = parent_tiles.shape[1]
        early = count - count // 2
        low, size = (0, early) if partial is None else (early, count - early)
        return update(low, size, words, parent_tiles[0], partial, cores, basis, flipped)

    sketch, updated = reduce_sketch(keep, sent, decode, incoming, owners, children)
    return updated[None], sketch.T


def solution(mesh):
    return jax.shard_map(
        shards,
        mesh=mesh,
        in_specs=(
            P("child", "tile", None, None),
            P("child", "tile", None),
            P("child", "tile", None),
            P("child", None, None),
            P("child", None, None),
            P("child", None),
            P("child", "tile", None, None),
            P("child", "tile", None),
            P(),
        ),
        out_specs=(P("child", "tile", None, None), P(("child", "tile"), None)),
        check_vma=False,
    )
```

```python
import jax
import jax.numpy as jnp
from jax import lax
from jax.experimental import pallas as pl
from jax.experimental.pallas import tpu as pltpu
from jax.sharding import PartitionSpec as P

CAP = 2
RING_OWNERS = 8
VMEM_BYTES = 58 * 1024 * 1024
STAGE_BYTES = 48 * 1024 * 1024
F32 = jnp.float32
BF16 = jnp.bfloat16
NT = (((1,), (1,)), ((), ()))


def dot(x, y):
    return jnp.dot(x, y, preferred_element_type=F32)


def params(size=VMEM_BYTES):
    return pltpu.CompilerParams(vmem_limit_bytes=size)


def project_kernel(panel_ref, basis_ref, out_ref):
    rank = basis_ref.shape[2]
    flipped = basis_ref[0].T
    out_ref[0, :rank] = flipped
    out_ref[0, rank:] = dot(flipped, panel_ref[0]).astype(BF16)


def project(panel, bases, order):
    blocks = panel.shape[0] // order
    width, rank = panel.shape[1], bases.shape[1]
    return pl.pallas_call(
        project_kernel,
        grid=(blocks,),
        in_specs=[
            pl.BlockSpec((1, order, width), lambda b: (b, 0, 0)),
            pl.BlockSpec((1, order, rank), lambda b: (b, 0, 0)),
        ],
        out_specs=pl.BlockSpec((1, 2 * rank, order), lambda b: (b, 0, 0)),
        out_shape=jax.ShapeDtypeStruct((blocks, 2 * rank, order), BF16),
        compiler_params=params(),
        name="project",
    )(panel.reshape(blocks, order, width), bases.reshape(blocks, order, rank))


def along_chips(x, owners, shift):
    return lax.ppermute(x, "tile", [(t, (t + 2 * shift) % owners) for t in range(owners)])


def to_partner(x, owners):
    return lax.ppermute(x, "tile", [(t, t ^ 1) for t in range(owners)])


def spread(block, tiles, owners):
    if owners > RING_OWNERS or owners % 4:
        return [lax.all_gather(block, "tile", axis=0, tiled=True)], None, stage(tiles)
    far, half = owners // 4, block.shape[1] // 2
    arrays, places = [block], [(0, 0)]
    up, down = block, block
    for step in range(1, far + 1):
        if step == far:
            up, down = up[:, :half], down[:, half:]
        up, down = along_chips(up, owners, 1), along_chips(down, owners, -1)
        arrays += [up, down]
        places += [(-step, 0), (step, half if step == far else 0)]
    return arrays + [to_partner(x, owners) for x in arrays], places, stage(tiles)


def grouped(count):
    return 4 if count % 4 == 0 else 1


def unpack(word, blocks):
    rest = word // blocks
    return rest // blocks, rest % blocks, word % blocks


SCALARS = pl.BlockSpec(memory_space=pltpu.SMEM)
ANYWHERE = pl.BlockSpec(memory_space=pl.ANY)
IN_HBM = pl.BlockSpec(memory_space=pltpu.HBM)
ON_CHIP = pl.BlockSpec(memory_space=pltpu.VMEM)


def stage_kernel(tiles, staged, sems):
    copies = [
        pltpu.make_async_copy(tiles.at[q], staged.at[q], sems.at[q])
        for q in range(tiles.shape[0])
    ]
    for copy in copies:
        copy.start()
    for copy in copies:
        copy.wait()


def stage(tiles):
    return pl.pallas_call(
        stage_kernel,
        in_specs=[IN_HBM],
        out_specs=ON_CHIP,
        scratch_shapes=[pltpu.SemaphoreType.DMA((tiles.shape[0],))],
        out_shape=pltpu.VMEM(tiles.shape, BF16),
        compiler_params=params(STAGE_BYTES),
        cost_estimate=pl.CostEstimate(
            flops=64 * tiles.size, bytes_accessed=4 * tiles.size, transcendentals=0
        ),
        name="stage",
    )(tiles)


def encode_kernel(places, count, words, staged, *refs):
    parts = refs[:-9]
    core_out, flip_out = refs[-9:-7]
    held, crossed, part_sems, core_sems, flip_sem = refs[-7:-2]
    coded = refs[-2]
    blocks = held.shape[0]
    rank = core_out.shape[1]
    flip_copy = pltpu.make_async_copy(held.at[:, :rank], flip_out, flip_sem)

    def part_copies():
        if places is None:
            return [pltpu.make_async_copy(parts[0], held, part_sems.at[0])]
        local = parts[0].shape[0]
        me = lax.axis_index("tile")
        chips = lax.axis_size("tile") // 2
        chip, core = me // 2, me % 2
        copies = []
        for n, part in enumerate(parts):
            offset, first = places[n % len(places)]
            owner = ((chip + chips + offset) % chips) * 2
            owner = owner + (core if n < len(places) else 1 - core)
            copies.append(
                pltpu.make_async_copy(
                    part,
                    held.at[pl.ds(owner * local, local), pl.ds(first, part.shape[1])],
                    part_sems.at[n],
                )
            )
        return copies

    def core_copy(q, place):
        return pltpu.make_async_copy(coded.at[q], core_out.at[place], core_sems.at[q])

    copies = part_copies()
    for copy in copies:
        copy.start()
    for copy in copies:
        copy.wait()
    flip_copy.start()

    group = grouped(count)

    def cross(g, carry):
        for q in [g * group + n for n in range(group)]:
            _, row, col = unpack(words[q], blocks)
            crossed[q] = lax.dot_general(
                held[row, rank:], held[col, rank:], NT, preferred_element_type=F32
            )
        return carry

    def one(g, carry):
        tiles_now = [g * group + n for n in range(group)]
        keys = [unpack(words[q], blocks) for q in tiles_now]
        halves = [
            dot(held[row, :rank], staged[q]).astype(BF16)
            for q, (_, row, _) in zip(tiles_now, keys)
        ]
        cores = [
            lax.dot_general(half, held[col, :rank], NT, preferred_element_type=F32)
            for half, (_, _, col) in zip(halves, keys)
        ]
        for q, core in zip(tiles_now, cores):
            coded[q] = (core - crossed[q]).astype(BF16)
        for q, (place, _, _) in zip(tiles_now, keys):
            core_copy(q, place).start()
        return carry

    lax.fori_loop(0, count // group, cross, 0)
    lax.fori_loop(0, count // group, one, 0)
    for q in range(count):
        core_copy(q, 0).wait()
    flip_copy.wait()


def encode(tiles, parts, places, words, owners):
    count, order, _ = tiles.shape
    rank = parts[0].shape[1] // 2
    blocks = parts[0].shape[0] * (1 if places is None else owners)
    slots = owners * CAP

    def body(words, staged, *refs):
        encode_kernel(places, count, words, staged, *refs, None)

    return pl.pallas_call(
        body,
        in_specs=[SCALARS, ON_CHIP] + [ANYWHERE] * len(parts),
        out_specs=[ANYWHERE, ANYWHERE],
        scratch_shapes=[
            pltpu.VMEM((blocks, 2 * rank, order), BF16),
            pltpu.VMEM((count, rank, rank), F32),
            pltpu.SemaphoreType.DMA((len(parts),)),
            pltpu.SemaphoreType.DMA((count,)),
            pltpu.SemaphoreType.DMA,
            pltpu.VMEM((count, rank, rank), BF16),
        ],
        out_shape=[
            jax.ShapeDtypeStruct((slots, rank, rank), BF16),
            jax.ShapeDtypeStruct((blocks, rank, order), BF16),
        ],
        compiler_params=params(VMEM_BYTES // 2),
        name="encode",
    )(words, tiles, *parts)


def add_rows(sketch, block, value):
    lanes = sketch.shape[2]
    pieces = value.shape[1] // lanes
    for r in range(pieces):
        sketch[block * pieces + r] += value[:, r * lanes : (r + 1) * lanes]


def prepare_kernel(words, pwords, flip_ref, test_ref, parents, basis_ref, west, vest, sketch, turned):
    blocks, tests = flip_ref.shape[0], test_ref.shape[0]
    count = parents.shape[0]
    sketch[...] = jnp.zeros_like(sketch)
    for b in range(tests):
        turned[b] = test_ref[b].T
    for b in range(blocks):
        basis_ref[b] = flip_ref[b].T

    def parent(p, carry):
        prow, pcol = pwords[2 * p], pwords[2 * p + 1]
        add_rows(
            sketch,
            prow,
            lax.dot_general(turned[pcol], parents[p], NT, preferred_element_type=F32),
        )

        @pl.when(prow != pcol)
        def _():
            add_rows(sketch, pcol, dot(turned[prow], parents[p]))

        return carry

    lax.fori_loop(0, count, parent, 0)

    group = grouped(west.shape[0])

    def item(g, carry):
        for s in [g * group + n for n in range(group)]:
            slot, row, col = unpack(words[s], blocks)
            at = 2 * jnp.maximum(slot - 1, 0)
            west[s] = lax.dot_general(
                turned[pwords[at + 1]], flip_ref[col], NT, preferred_element_type=F32
            ).astype(BF16)
            vest[s] = lax.dot_general(
                turned[pwords[at]], flip_ref[row], NT, preferred_element_type=F32
            ).astype(BF16)
        return carry

    lax.fori_loop(0, west.shape[0] // group, item, 0)


def prepare(words, pwords, flipped, test, parents, lanes):
    blocks, rank, order = flipped.shape
    tests, _, width = test.shape
    items = words.shape[0]
    return pl.pallas_call(
        prepare_kernel,
        in_specs=[SCALARS, SCALARS, ON_CHIP, ON_CHIP, ON_CHIP],
        out_specs=[ON_CHIP] * 4,
        scratch_shapes=[pltpu.VMEM((tests, width, order), BF16)],
        out_shape=[
            jax.ShapeDtypeStruct((blocks, order, rank), BF16),
            jax.ShapeDtypeStruct((items, width, rank), BF16),
            jax.ShapeDtypeStruct((items, width, rank), BF16),
            jax.ShapeDtypeStruct((tests * order // lanes, width, lanes), F32),
        ],
        compiler_params=params(VMEM_BYTES),
        cost_estimate=pl.CostEstimate(
            flops=4 * parents.size * width, bytes_accessed=2 * parents.size, transcendentals=0
        ),
        name="prepare",
    )(words, pwords, flipped, test, parents)


def fold_kernel(
    words, pwords, core_ref, west, vest, flip_ref, start, keep_ref, send_ref, sketch, base, sem
):
    blocks = flip_ref.shape[0]
    base_copy = pltpu.make_async_copy(start, base, sem)
    base_copy.start()
    sketch[...] = jnp.zeros_like(sketch)

    group = grouped(core_ref.shape[0])

    def item(g, carry):
        targets, values = [], []
        for s in [g * group + n for n in range(group)]:
            slot, row, col = unpack(words[s], blocks)
            at = 2 * jnp.maximum(slot - 1, 0)
            prow, pcol = pwords[at], pwords[at + 1]
            core = jnp.where(slot > 0, core_ref[s], jnp.zeros_like(core_ref[s]))
            first = lax.dot_general(west[s], core, NT, preferred_element_type=F32)
            second = jnp.where(prow != pcol, dot(vest[s], core), 0.0)
            targets += [prow, pcol]
            values += [(first.astype(BF16), row), (second.astype(BF16), col)]
        values = [dot(value, flip_ref[block]) for value, block in values]
        for target, value in zip(targets, values):
            add_rows(sketch, target, value)
        return carry

    lax.fori_loop(0, core_ref.shape[0] // group, item, 0)
    base_copy.wait()
    core = lax.axis_index("tile") % 2
    for n in range(keep_ref.shape[0]):
        mine, other = 2 * n + core, 2 * n + 1 - core
        keep_ref[n] = (sketch[mine] + base[mine]).astype(BF16)
        send_ref[n] = (sketch[other] + base[other]).astype(BF16)


def fold(words, pwords, cores, west, vest, flipped, start):
    chunks, width, lanes = start.shape
    half = jax.ShapeDtypeStruct((chunks // 2, width, lanes), BF16)
    return pl.pallas_call(
        fold_kernel,
        in_specs=[SCALARS, SCALARS] + [ON_CHIP] * 4 + [ANYWHERE],
        out_specs=[ON_CHIP, ON_CHIP],
        scratch_shapes=[
            pltpu.VMEM(start.shape, F32),
            pltpu.VMEM(start.shape, F32),
            pltpu.SemaphoreType.DMA,
        ],
        out_shape=[half, half],
        compiler_params=params(VMEM_BYTES),
        name="fold",
    )(words, pwords, cores, west, vest, flipped, start)


def update_kernel(
    words, parents, core_in, flip_in, basis_in, updated,
    cores, flips, basis, held, total, mixed, sems, in_sems, out_sems,
):
    count, blocks, items = held.shape[0], basis.shape[0], cores.shape[0]
    group = grouped(items)
    loads = [
        pltpu.make_async_copy(source, target, sems.at[n])
        for n, (source, target) in enumerate(
            ((core_in, cores), (flip_in, flips), (basis_in, basis))
        )
    ]

    def in_copy(p):
        return pltpu.make_async_copy(parents.at[p], held.at[p], in_sems.at[p])

    def out_copy(p):
        return pltpu.make_async_copy(held.at[p], updated.at[p], out_sems.at[p])

    for load in loads:
        load.start()
    for p in range(count):
        in_copy(p).start()
    loads[0].wait()
    loads[1].wait()

    def mix(g, carry):
        for s in [g * group + n for n in range(group)]:
            _, _, col = unpack(words[s], blocks)
            mixed[s] = dot(cores[s], flips[col]).astype(BF16)
        return carry

    lax.fori_loop(0, items // group, mix, 0)
    loads[2].wait()

    def one(p, carry):
        in_copy(p).wait()
        total[...] = held[p].astype(F32)

        def item(s, carry):
            slot, row, _ = unpack(words[s], blocks)

            @pl.when(slot == p + 1)
            def _():
                total[...] += dot(basis[row], mixed[s])

            return carry

        lax.fori_loop(0, items, item, 0)
        held[p] = total[...].astype(BF16)
        out_copy(p).start()
        return carry

    lax.fori_loop(0, count, one, 0)
    for p in range(count):
        out_copy(p).wait()


def update(words, parents, cores, basis, flipped):
    count, order, _ = parents.shape
    rank = basis.shape[2]
    return pl.pallas_call(
        update_kernel,
        in_specs=[SCALARS, IN_HBM] + [ANYWHERE] * 3,
        out_specs=IN_HBM,
        scratch_shapes=[
            pltpu.VMEM(cores.shape, BF16),
            pltpu.VMEM(flipped.shape, BF16),
            pltpu.VMEM(basis.shape, BF16),
            pltpu.VMEM(parents.shape, BF16),
            pltpu.VMEM((order, order), F32),
            pltpu.VMEM((cores.shape[0], rank, order), BF16),
            pltpu.SemaphoreType.DMA((3,)),
            pltpu.SemaphoreType.DMA((count,)),
            pltpu.SemaphoreType.DMA((count,)),
        ],
        out_shape=jax.ShapeDtypeStruct(parents.shape, BF16),
        compiler_params=params(),
        cost_estimate=pl.CostEstimate(
            flops=8 * parents.size * rank, bytes_accessed=4 * parents.size, transcendentals=0
        ),
        name="update",
    )(words, parents, cores, flipped, basis)


def partner(i, step, size):
    return i ^ step if size & (size - 1) == 0 else (i + step) % size


def exchange_sum(pieces, size, me, send, group):
    mine = lax.dynamic_slice_in_dim(pieces, me * group, group, 0)
    for shift in range(1, size):
        peer = partner(me, shift, size)
        out = lax.dynamic_slice_in_dim(pieces, peer * group, group, 0).astype(BF16)
        mine = mine + send(out, shift).astype(F32)
    return mine


def reduce_sketch(keep, sent, updated, owners, children):
    child, tile = lax.axis_index("child"), lax.axis_index("tile")
    chips = owners // 2
    pieces = keep.astype(F32) + to_partner(sent, owners).astype(F32)

    def over_child(x, shift):
        return lax.ppermute(
            x, "child", [(i, partner(i, shift, children)) for i in range(children)]
        )

    def over_chips(x, shift):
        return lax.ppermute(
            x, "tile", [(t, 2 * partner(t // 2, shift, chips) + t % 2) for t in range(owners)]
        )

    pieces = exchange_sum(pieces, children, child, over_child, chips)
    pieces, updated = lax.optimization_barrier((pieces, updated))
    return exchange_sum(pieces, chips, tile // 2, over_chips, 1)[0], updated


def shards(
    child_tiles,
    panel,
    bases,
    tile_blocks,
    tile_dest,
    tile_slot,
    parent_tiles,
    parent_blocks,
    sketch_test,
):
    owners, children = lax.axis_size("tile"), lax.axis_size("child")
    myself = lax.axis_index("tile")
    tile_count, order = child_tiles.shape[1], child_tiles.shape[2]

    block = project(panel[0], bases[0], order)
    parts, places, staged = spread(block, child_tiles[0], owners)

    blocks = owners * panel.shape[1] // order
    pair_all = (tile_blocks[0, :, 0] * blocks + tile_blocks[0, :, 1]).reshape(owners, tile_count)
    dest_all = tile_dest[0, :, 0].reshape(owners, tile_count)
    own_pair = lax.dynamic_index_in_dim(pair_all, myself, 0, keepdims=False)
    own_dest = lax.dynamic_index_in_dim(dest_all, myself, 0, keepdims=False)
    ids = jnp.arange(tile_count, dtype=jnp.int32)
    lower = ids[None, :] < ids[:, None]
    before = (own_dest[:, None] == own_dest[None, :]) & lower
    place = own_dest * CAP + jnp.sum(before.astype(jnp.int32), axis=1)
    own_words = place * (blocks * blocks) + own_pair

    arrive = dest_all == myself
    earlier = jnp.sum((arrive[:, None, :] & lower[None]).astype(jnp.int32), axis=2)
    turn = jnp.arange(CAP, dtype=jnp.int32)
    matched = arrive[:, None, :] & (earlier[:, None, :] == turn[None, :, None])
    word_all = (tile_slot[0].reshape(owners, tile_count) + 1) * (blocks * blocks) + pair_all
    words = jnp.sum(jnp.where(matched, word_all[:, None, :], 0), axis=2).reshape(-1)
    pwords = parent_blocks[0].reshape(-1)

    cores, flipped = encode(staged, parts, places, own_words, owners)
    rank = cores.shape[1]
    incoming = lax.all_to_all(
        cores.reshape(owners, CAP, rank, rank), "tile", split_axis=0, concat_axis=0, tiled=True
    ).reshape(cores.shape)
    width = sketch_test.shape[1]
    lanes = sketch_test.shape[0] // (owners * children)
    basis, west, vest, start = prepare(
        words, pwords, flipped, sketch_test.reshape(-1, order, width), parent_tiles[0], lanes
    )
    keep, sent = fold(words, pwords, incoming, west, vest, flipped, start)
    updated = update(words, parent_tiles[0], incoming, basis, flipped)
    sketch, updated = reduce_sketch(keep, sent, updated, owners, children)
    return updated[None], sketch.T


def solution(mesh):
    return jax.shard_map(
        shards,
        mesh=mesh,
        in_specs=(
            P("child", "tile", None, None),
            P("child", "tile", None),
            P("child", "tile", None),
            P("child", None, None),
            P("child", None, None),
            P("child", None),
            P("child", "tile", None, None),
            P("child", "tile", None),
            P(),
        ),
        out_specs=(P("child", "tile", None, None), P(("child", "tile"), None)),
        check_vma=False,
    )
```

```python
import jax
import jax.numpy as jnp
from jax import lax
from jax.experimental import pallas as pl
from jax.experimental.pallas import tpu as pltpu
from jax.sharding import PartitionSpec as P

CAP = 2
BITS = 10
RING_OWNERS = 8
VMEM_BYTES = 58 * 1024 * 1024
STAGE_BYTES = 48 * 1024 * 1024
F32 = jnp.float32
BF16 = jnp.bfloat16
NT = (((1,), (1,)), ((), ()))


def dot(x, y):
    return jnp.dot(x, y, preferred_element_type=F32)


def params(size=VMEM_BYTES):
    return pltpu.CompilerParams(vmem_limit_bytes=size)


def project_kernel(panel_ref, basis_ref, out_ref):
    rank = basis_ref.shape[2]
    flipped = basis_ref[0].T
    out_ref[0, :rank] = flipped
    out_ref[0, rank:] = dot(flipped, panel_ref[0]).astype(BF16)


def project(panel, bases, order):
    blocks = panel.shape[0] // order
    width, rank = panel.shape[1], bases.shape[1]
    return pl.pallas_call(
        project_kernel,
        grid=(blocks,),
        in_specs=[
            pl.BlockSpec((1, order, width), lambda b: (b, 0, 0)),
            pl.BlockSpec((1, order, rank), lambda b: (b, 0, 0)),
        ],
        out_specs=pl.BlockSpec((1, 2 * rank, order), lambda b: (b, 0, 0)),
        out_shape=jax.ShapeDtypeStruct((blocks, 2 * rank, order), BF16),
        compiler_params=params(),
        name="project",
    )(panel.reshape(blocks, order, width), bases.reshape(blocks, order, rank))


def along_chips(x, owners, shift):
    return lax.ppermute(x, "tile", [(t, (t + 2 * shift) % owners) for t in range(owners)])


def to_partner(x, owners):
    return lax.ppermute(x, "tile", [(t, t ^ 1) for t in range(owners)])


def spread(block, tiles, owners):
    if owners > RING_OWNERS or owners % 4:
        return [lax.all_gather(block, "tile", axis=0, tiled=True)], None, stage(tiles)
    far, half = owners // 4, block.shape[1] // 2
    arrays, places = [block], [(0, 0)]
    up, down = block, block
    for step in range(1, far + 1):
        if step == far:
            up, down = up[:, :half], down[:, half:]
        up, down = along_chips(up, owners, 1), along_chips(down, owners, -1)
        arrays += [up, down]
        places += [(-step, 0), (step, half if step == far else 0)]
    return arrays + [to_partner(x, owners) for x in arrays], places, stage(tiles)


def grouped(count):
    return 4 if count % 4 == 0 else 1


def pack(place, row, col):
    return (place << (2 * BITS)) | (row << BITS) | col


def unpack(word):
    low = (1 << BITS) - 1
    return word >> (2 * BITS), (word >> BITS) & low, word & low


SCALARS = pl.BlockSpec(memory_space=pltpu.SMEM)
ANYWHERE = pl.BlockSpec(memory_space=pl.ANY)
IN_HBM = pl.BlockSpec(memory_space=pltpu.HBM)
ON_CHIP = pl.BlockSpec(memory_space=pltpu.VMEM)


def stage_kernel(tiles, staged, sems):
    copies = [
        pltpu.make_async_copy(tiles.at[q], staged.at[q], sems.at[q])
        for q in range(tiles.shape[0])
    ]
    for copy in copies:
        copy.start()
    for copy in copies:
        copy.wait()


def stage(tiles):
    return pl.pallas_call(
        stage_kernel,
        in_specs=[IN_HBM],
        out_specs=ON_CHIP,
        scratch_shapes=[pltpu.SemaphoreType.DMA((tiles.shape[0],))],
        out_shape=pltpu.VMEM(tiles.shape, BF16),
        compiler_params=params(STAGE_BYTES),
        cost_estimate=pl.CostEstimate(
            flops=64 * tiles.size, bytes_accessed=4 * tiles.size, transcendentals=0
        ),
        name="stage",
    )(tiles)


def encode_kernel(places, count, words, staged, *refs):
    parts = refs[:-9]
    core_out, flip_out = refs[-9:-7]
    held, crossed, part_sems, core_sems, flip_sem = refs[-7:-2]
    coded = refs[-2]
    rank = core_out.shape[1]
    flip_copy = pltpu.make_async_copy(held.at[:, :rank], flip_out, flip_sem)

    def part_copies():
        if places is None:
            return [pltpu.make_async_copy(parts[0], held, part_sems.at[0])]
        local = parts[0].shape[0]
        me = lax.axis_index("tile")
        chips = lax.axis_size("tile") // 2
        chip, core = me // 2, me % 2
        copies = []
        for n, part in enumerate(parts):
            offset, first = places[n % len(places)]
            owner = ((chip + chips + offset) % chips) * 2
            owner = owner + (core if n < len(places) else 1 - core)
            copies.append(
                pltpu.make_async_copy(
                    part,
                    held.at[pl.ds(owner * local, local), pl.ds(first, part.shape[1])],
                    part_sems.at[n],
                )
            )
        return copies

    def core_copy(q, place):
        return pltpu.make_async_copy(coded.at[q], core_out.at[place], core_sems.at[q])

    copies = part_copies()
    for copy in copies:
        copy.start()
    for copy in copies:
        copy.wait()
    flip_copy.start()

    group = grouped(count)

    def cross(g, carry):
        for q in [g * group + n for n in range(group)]:
            _, row, col = unpack(words[q])
            crossed[q] = lax.dot_general(
                held[row, rank:], held[col, rank:], NT, preferred_element_type=F32
            )
        return carry

    def one(g, carry):
        tiles_now = [g * group + n for n in range(group)]
        keys = [unpack(words[q]) for q in tiles_now]
        halves = [
            dot(held[row, :rank], staged[q]).astype(BF16)
            for q, (_, row, _) in zip(tiles_now, keys)
        ]
        cores = [
            lax.dot_general(half, held[col, :rank], NT, preferred_element_type=F32)
            for half, (_, _, col) in zip(halves, keys)
        ]
        for q, core in zip(tiles_now, cores):
            coded[q] = (core - crossed[q]).astype(BF16)
        for q, (place, _, _) in zip(tiles_now, keys):
            core_copy(q, place).start()
        return carry

    lax.fori_loop(0, count // group, cross, 0)
    lax.fori_loop(0, count // group, one, 0)
    for q in range(count):
        core_copy(q, 0).wait()
    flip_copy.wait()


def encode(tiles, parts, places, words, owners):
    count, order, _ = tiles.shape
    rank = parts[0].shape[1] // 2
    blocks = parts[0].shape[0] * (1 if places is None else owners)
    slots = owners * CAP

    def body(words, staged, *refs):
        encode_kernel(places, count, words, staged, *refs, None)

    return pl.pallas_call(
        body,
        in_specs=[SCALARS, ON_CHIP] + [ANYWHERE] * len(parts),
        out_specs=[ANYWHERE, ANYWHERE],
        scratch_shapes=[
            pltpu.VMEM((blocks, 2 * rank, order), BF16),
            pltpu.VMEM((count, rank, rank), F32),
            pltpu.SemaphoreType.DMA((len(parts),)),
            pltpu.SemaphoreType.DMA((count,)),
            pltpu.SemaphoreType.DMA,
            pltpu.VMEM((count, rank, rank), BF16),
        ],
        out_shape=[
            jax.ShapeDtypeStruct((slots, rank, rank), BF16),
            pltpu.HBM((blocks, rank, order), BF16),
        ],
        compiler_params=params(VMEM_BYTES // 2),
        name="encode",
    )(words, tiles, *parts)


def add_rows(sketch, block, value):
    lanes = sketch.shape[2]
    pieces = value.shape[1] // lanes
    for r in range(pieces):
        sketch[block * pieces + r] += value[:, r * lanes : (r + 1) * lanes]


def prepare_kernel(words, pwords, flip_ref, test_ref, parents, basis_ref, west, vest, sketch, turned):
    blocks, tests = flip_ref.shape[0], test_ref.shape[0]
    count = parents.shape[0]
    sketch[...] = jnp.zeros_like(sketch)
    for b in range(tests):
        turned[b] = test_ref[b].T
    for b in range(blocks):
        basis_ref[b] = flip_ref[b].T

    def parent(p, carry):
        prow, pcol = pwords[2 * p], pwords[2 * p + 1]
        add_rows(
            sketch,
            prow,
            lax.dot_general(turned[pcol], parents[p], NT, preferred_element_type=F32),
        )

        @pl.when(prow != pcol)
        def _():
            add_rows(sketch, pcol, dot(turned[prow], parents[p]))

        return carry

    lax.fori_loop(0, count, parent, 0)

    group = grouped(west.shape[0])

    def item(g, carry):
        for s in [g * group + n for n in range(group)]:
            slot, row, col = unpack(words[s])
            at = 2 * jnp.maximum(slot - 1, 0)
            west[s] = lax.dot_general(
                turned[pwords[at + 1]], flip_ref[col], NT, preferred_element_type=F32
            ).astype(BF16)
            vest[s] = lax.dot_general(
                turned[pwords[at]], flip_ref[row], NT, preferred_element_type=F32
            ).astype(BF16)
        return carry

    lax.fori_loop(0, west.shape[0] // group, item, 0)


def prepare(words, pwords, flipped, test, parents, lanes):
    blocks, rank, order = flipped.shape
    tests, _, width = test.shape
    items = words.shape[0]
    return pl.pallas_call(
        prepare_kernel,
        in_specs=[SCALARS, SCALARS, ON_CHIP, ON_CHIP, ON_CHIP],
        out_specs=[ON_CHIP] * 4,
        scratch_shapes=[pltpu.VMEM((tests, width, order), BF16)],
        out_shape=[
            jax.ShapeDtypeStruct((blocks, order, rank), BF16),
            jax.ShapeDtypeStruct((items, width, rank), BF16),
            jax.ShapeDtypeStruct((items, width, rank), BF16),
            jax.ShapeDtypeStruct((tests * order // lanes, width, lanes), F32),
        ],
        compiler_params=params(VMEM_BYTES),
        cost_estimate=pl.CostEstimate(
            flops=4 * parents.size * width, bytes_accessed=2 * parents.size, transcendentals=0
        ),
        name="prepare",
    )(words, pwords, flipped, test, parents)


def fold_kernel(
    words, pwords, core_ref, west, vest, flip_ref, start, keep_ref, send_ref, sketch, base, sem
):
    base_copy = pltpu.make_async_copy(start, base, sem)
    base_copy.start()
    sketch[...] = jnp.zeros_like(sketch)

    group = grouped(core_ref.shape[0])

    def item(g, carry):
        targets, values = [], []
        for s in [g * group + n for n in range(group)]:
            slot, row, col = unpack(words[s])
            at = 2 * jnp.maximum(slot - 1, 0)
            prow, pcol = pwords[at], pwords[at + 1]
            core = jnp.where(slot > 0, core_ref[s], jnp.zeros_like(core_ref[s]))
            first = lax.dot_general(west[s], core, NT, preferred_element_type=F32)
            second = jnp.where(prow != pcol, dot(vest[s], core), 0.0)
            targets += [prow, pcol]
            values += [(first.astype(BF16), row), (second.astype(BF16), col)]
        values = [dot(value, flip_ref[block]) for value, block in values]
        for target, value in zip(targets, values):
            add_rows(sketch, target, value)
        return carry

    lax.fori_loop(0, core_ref.shape[0] // group, item, 0)
    base_copy.wait()
    core = lax.axis_index("tile") % 2
    for n in range(keep_ref.shape[0]):
        mine, other = 2 * n + core, 2 * n + 1 - core
        keep_ref[n] = (sketch[mine] + base[mine]).astype(BF16)
        send_ref[n] = (sketch[other] + base[other]).astype(BF16)


def fold(words, pwords, cores, west, vest, flipped, start):
    chunks, width, lanes = start.shape
    half = jax.ShapeDtypeStruct((chunks // 2, width, lanes), BF16)
    return pl.pallas_call(
        fold_kernel,
        in_specs=[SCALARS, SCALARS] + [ON_CHIP] * 4 + [ANYWHERE],
        out_specs=[ON_CHIP, ON_CHIP],
        scratch_shapes=[
            pltpu.VMEM(start.shape, F32),
            pltpu.VMEM(start.shape, F32),
            pltpu.SemaphoreType.DMA,
        ],
        out_shape=[half, half],
        compiler_params=params(VMEM_BYTES),
        name="fold",
    )(words, pwords, cores, west, vest, flipped, start)


def update_kernel(
    low, words, parents, partial, core_in, flip_in, basis_in, updated,
    cores, flips, basis, held, total, mixed, sems, in_sems, out_sems,
):
    count, items = held.shape[0], cores.shape[0]
    group = grouped(items)
    loads = [
        pltpu.make_async_copy(source, target, sems.at[n])
        for n, (source, target) in enumerate(
            ((core_in, cores), (flip_in, flips), (basis_in, basis))
        )
    ]

    def in_copy(p):
        return pltpu.make_async_copy(parents.at[low + p], held.at[p], in_sems.at[p])

    def out_copy(p):
        return pltpu.make_async_copy(held.at[p], updated.at[low + p], out_sems.at[p])

    for load in loads:
        load.start()
    for p in range(count):
        in_copy(p).start()
    loads[0].wait()
    loads[1].wait()

    def mix(g, carry):
        for s in [g * group + n for n in range(group)]:
            _, _, col = unpack(words[s])
            mixed[s] = dot(cores[s], flips[col]).astype(BF16)
        return carry

    lax.fori_loop(0, items // group, mix, 0)
    loads[2].wait()

    def one(p, carry):
        in_copy(p).wait()
        total[...] = held[p].astype(F32)

        def item(s, carry):
            slot, row, _ = unpack(words[s])

            @pl.when(slot == low + p + 1)
            def _():
                total[...] += dot(basis[row], mixed[s])

            return carry

        lax.fori_loop(0, items, item, 0)
        held[p] = total[...].astype(BF16)
        out_copy(p).start()
        return carry

    lax.fori_loop(0, count, one, 0)
    for p in range(count):
        out_copy(p).wait()


def update(low, count, words, parents, partial, cores, basis, flipped):
    order = parents.shape[1]
    rank = basis.shape[2]
    first = partial is None
    given = [] if first else [partial]

    def body(words, parents, *refs):
        update_kernel(low, words, parents, *([None] if first else []), *refs)

    return pl.pallas_call(
        body,
        in_specs=[SCALARS, IN_HBM] + [IN_HBM] * len(given) + [ANYWHERE] * 3,
        out_specs=IN_HBM,
        scratch_shapes=[
            pltpu.VMEM(cores.shape, BF16),
            pltpu.VMEM(flipped.shape, BF16),
            pltpu.VMEM(basis.shape, BF16),
            pltpu.VMEM((count, order, order), BF16),
            pltpu.VMEM((order, order), F32),
            pltpu.VMEM((cores.shape[0], rank, order), BF16),
            pltpu.SemaphoreType.DMA((3,)),
            pltpu.SemaphoreType.DMA((count,)),
            pltpu.SemaphoreType.DMA((count,)),
        ],
        out_shape=jax.ShapeDtypeStruct(parents.shape, BF16),
        input_output_aliases={} if first else {2: 0},
        compiler_params=params(),
        cost_estimate=pl.CostEstimate(
            flops=8 * parents.size * rank, bytes_accessed=4 * parents.size, transcendentals=0
        ),
        name="update",
    )(words, parents, *given, cores, flipped, basis)


def partner(i, step, size):
    return i ^ step if size & (size - 1) == 0 else (i + step) % size


def exchange_sum(pieces, size, me, send, group):
    mine = lax.dynamic_slice_in_dim(pieces, me * group, group, 0)
    for shift in range(1, size):
        peer = partner(me, shift, size)
        out = lax.dynamic_slice_in_dim(pieces, peer * group, group, 0).astype(BF16)
        mine = mine + send(out, shift).astype(F32)
    return mine


def reduce_sketch(keep, sent, decode, cores, owners, children):
    child, tile = lax.axis_index("child"), lax.axis_index("tile")
    chips = owners // 2
    pieces = keep.astype(F32) + to_partner(sent, owners).astype(F32)

    def over_child(x, shift):
        return lax.ppermute(
            x, "child", [(i, partner(i, shift, children)) for i in range(children)]
        )

    def over_chips(x, shift):
        return lax.ppermute(
            x, "tile", [(t, 2 * partner(t // 2, shift, chips) + t % 2) for t in range(owners)]
        )

    pieces = exchange_sum(pieces, children, child, over_child, chips)
    pieces, updated, cores = lax.optimization_barrier((pieces, decode(None, cores), cores))
    return exchange_sum(pieces, chips, tile // 2, over_chips, 1)[0], decode(updated, cores)


def shards(
    child_tiles,
    panel,
    bases,
    tile_blocks,
    tile_dest,
    tile_slot,
    parent_tiles,
    parent_blocks,
    sketch_test,
):
    owners, children = lax.axis_size("tile"), lax.axis_size("child")
    myself = lax.axis_index("tile")
    tile_count, order = child_tiles.shape[1], child_tiles.shape[2]

    block = project(panel[0], bases[0], order)
    parts, places, staged = spread(block, child_tiles[0], owners)

    pair_all = pack(0, tile_blocks[0, :, 0], tile_blocks[0, :, 1]).reshape(owners, tile_count)
    dest_all = tile_dest[0, :, 0].reshape(owners, tile_count)
    own_pair = lax.dynamic_index_in_dim(pair_all, myself, 0, keepdims=False)
    own_dest = lax.dynamic_index_in_dim(dest_all, myself, 0, keepdims=False)
    ids = jnp.arange(tile_count, dtype=jnp.int32)
    lower = ids[None, :] < ids[:, None]
    before = (own_dest[:, None] == own_dest[None, :]) & lower
    place = own_dest * CAP + jnp.sum(before.astype(jnp.int32), axis=1)
    own_words = pack(place, 0, own_pair)

    arrive = dest_all == myself
    earlier = jnp.sum((arrive[:, None, :] & lower[None]).astype(jnp.int32), axis=2)
    turn = jnp.arange(CAP, dtype=jnp.int32)
    matched = arrive[:, None, :] & (earlier[:, None, :] == turn[None, :, None])
    word_all = pack(tile_slot[0].reshape(owners, tile_count) + 1, 0, pair_all)
    words = jnp.sum(jnp.where(matched, word_all[:, None, :], 0), axis=2).reshape(-1)
    pwords = parent_blocks[0].reshape(-1)

    cores, flipped = encode(staged, parts, places, own_words, owners)
    rank = cores.shape[1]
    incoming = lax.all_to_all(
        cores.reshape(owners, CAP, rank, rank), "tile", split_axis=0, concat_axis=0, tiled=True
    ).reshape(cores.shape)
    width = sketch_test.shape[1]
    lanes = sketch_test.shape[0] // (owners * children)
    basis, west, vest, start = prepare(
        words, pwords, flipped, sketch_test.reshape(-1, order, width), parent_tiles[0], lanes
    )
    keep, sent = fold(words, pwords, incoming, west, vest, flipped, start)

    def decode(partial, cores):
        count = parent_tiles.shape[1]
        early = count - count * 3 // 8
        low, size = (0, early) if partial is None else (early, count - early)
        return update(low, size, words, parent_tiles[0], partial, cores, basis, flipped)

    sketch, updated = reduce_sketch(keep, sent, decode, incoming, owners, children)
    return updated[None], sketch.T


def solution(mesh):
    return jax.shard_map(
        shards,
        mesh=mesh,
        in_specs=(
            P("child", "tile", None, None),
            P("child", "tile", None),
            P("child", "tile", None),
            P("child", None, None),
            P("child", None, None),
            P("child", None),
            P("child", "tile", None, None),
            P("child", "tile", None),
            P(),
        ),
        out_specs=(P("child", "tile", None, None), P(("child", "tile"), None)),
        check_vma=False,
    )
```

```python
import jax
import jax.numpy as jnp
from jax import lax
from jax.experimental import pallas as pl
from jax.experimental.pallas import tpu as pltpu
from jax.sharding import PartitionSpec as P

CAP = 2
BITS = 10
RING_OWNERS = 8
VMEM_BYTES = 58 * 1024 * 1024
STAGE_BYTES = 48 * 1024 * 1024
F32 = jnp.float32
BF16 = jnp.bfloat16
NT = (((1,), (1,)), ((), ()))


def dot(x, y):
    return jnp.dot(x, y, preferred_element_type=F32)


def params(size=VMEM_BYTES):
    return pltpu.CompilerParams(vmem_limit_bytes=size)


def project_kernel(panel_ref, basis_ref, out_ref):
    rank = basis_ref.shape[2]
    flipped = basis_ref[0].T
    out_ref[0, :rank] = flipped
    out_ref[0, rank:] = dot(flipped, panel_ref[0]).astype(BF16)


def project(panel, bases, order):
    blocks = panel.shape[0] // order
    width, rank = panel.shape[1], bases.shape[1]
    return pl.pallas_call(
        project_kernel,
        grid=(blocks,),
        in_specs=[
            pl.BlockSpec((1, order, width), lambda b: (b, 0, 0)),
            pl.BlockSpec((1, order, rank), lambda b: (b, 0, 0)),
        ],
        out_specs=pl.BlockSpec((1, 2 * rank, order), lambda b: (b, 0, 0)),
        out_shape=jax.ShapeDtypeStruct((blocks, 2 * rank, order), BF16),
        compiler_params=params(),
        name="project",
    )(panel.reshape(blocks, order, width), bases.reshape(blocks, order, rank))


def along_chips(x, owners, shift):
    return lax.ppermute(x, "tile", [(t, (t + 2 * shift) % owners) for t in range(owners)])


def to_partner(x, owners):
    return lax.ppermute(x, "tile", [(t, t ^ 1) for t in range(owners)])


def spread(block, tiles, owners):
    if owners > RING_OWNERS or owners % 4:
        return [lax.all_gather(block, "tile", axis=0, tiled=True)], None, stage(tiles)
    far, half = owners // 4, block.shape[1] // 2
    arrays, places = [block], [(0, 0)]
    up, down = block, block
    for step in range(1, far + 1):
        if step == far:
            up, down = up[:, :half], down[:, half:]
        up, down = along_chips(up, owners, 1), along_chips(down, owners, -1)
        arrays += [up, down]
        places += [(-step, 0), (step, half if step == far else 0)]
    return arrays + [to_partner(x, owners) for x in arrays], places, stage(tiles)


def grouped(count):
    return 4 if count % 4 == 0 else 1


def pack(place, row, col):
    return (place << (2 * BITS)) | (row << BITS) | col


def unpack(word):
    low = (1 << BITS) - 1
    return word >> (2 * BITS), (word >> BITS) & low, word & low


SCALARS = pl.BlockSpec(memory_space=pltpu.SMEM)
ANYWHERE = pl.BlockSpec(memory_space=pl.ANY)
IN_HBM = pl.BlockSpec(memory_space=pltpu.HBM)
ON_CHIP = pl.BlockSpec(memory_space=pltpu.VMEM)


def stage_kernel(tiles, staged, sems):
    copies = [
        pltpu.make_async_copy(tiles.at[q], staged.at[q], sems.at[q])
        for q in range(tiles.shape[0])
    ]
    for copy in copies:
        copy.start()
    for copy in copies:
        copy.wait()


def stage(tiles):
    return pl.pallas_call(
        stage_kernel,
        in_specs=[IN_HBM],
        out_specs=ON_CHIP,
        scratch_shapes=[pltpu.SemaphoreType.DMA((tiles.shape[0],))],
        out_shape=pltpu.VMEM(tiles.shape, BF16),
        compiler_params=params(STAGE_BYTES),
        cost_estimate=pl.CostEstimate(
            flops=64 * tiles.size, bytes_accessed=4 * tiles.size, transcendentals=0
        ),
        name="stage",
    )(tiles)


def encode_kernel(places, count, words, staged, *refs):
    parts = refs[:-9]
    core_out, flip_out = refs[-9:-7]
    held, crossed, part_sems, core_sems, flip_sem = refs[-7:-2]
    coded = refs[-2]
    rank = core_out.shape[1]
    flip_copy = pltpu.make_async_copy(held.at[:, :rank], flip_out, flip_sem)

    def part_copies():
        if places is None:
            return [pltpu.make_async_copy(parts[0], held, part_sems.at[0])]
        local = parts[0].shape[0]
        me = lax.axis_index("tile")
        chips = lax.axis_size("tile") // 2
        chip, core = me // 2, me % 2
        copies = []
        for n, part in enumerate(parts):
            offset, first = places[n % len(places)]
            owner = ((chip + chips + offset) % chips) * 2
            owner = owner + (core if n < len(places) else 1 - core)
            copies.append(
                pltpu.make_async_copy(
                    part,
                    held.at[pl.ds(owner * local, local), pl.ds(first, part.shape[1])],
                    part_sems.at[n],
                )
            )
        return copies

    def core_copy(q, place):
        return pltpu.make_async_copy(coded.at[q], core_out.at[place], core_sems.at[q])

    copies = part_copies()
    for copy in copies:
        copy.start()
    for copy in copies:
        copy.wait()
    flip_copy.start()

    group = grouped(count)

    def cross(g, carry):
        for q in [g * group + n for n in range(group)]:
            _, row, col = unpack(words[q])
            crossed[q] = lax.dot_general(
                held[row, rank:], held[col, rank:], NT, preferred_element_type=F32
            )
        return carry

    def one(g, carry):
        tiles_now = [g * group + n for n in range(group)]
        keys = [unpack(words[q]) for q in tiles_now]
        halves = [
            dot(held[row, :rank], staged[q]).astype(BF16)
            for q, (_, row, _) in zip(tiles_now, keys)
        ]
        cores = [
            lax.dot_general(half, held[col, :rank], NT, preferred_element_type=F32)
            for half, (_, _, col) in zip(halves, keys)
        ]
        for q, core in zip(tiles_now, cores):
            coded[q] = (core - crossed[q]).astype(BF16)
        for q, (place, _, _) in zip(tiles_now, keys):
            core_copy(q, place).start()
        return carry

    lax.fori_loop(0, count // group, cross, 0)
    lax.fori_loop(0, count // group, one, 0)
    for q in range(count):
        core_copy(q, 0).wait()
    flip_copy.wait()


def encode(tiles, parts, places, words, owners):
    count, order, _ = tiles.shape
    rank = parts[0].shape[1] // 2
    blocks = parts[0].shape[0] * (1 if places is None else owners)
    slots = owners * CAP

    def body(words, staged, *refs):
        encode_kernel(places, count, words, staged, *refs, None)

    return pl.pallas_call(
        body,
        in_specs=[SCALARS, ON_CHIP] + [ANYWHERE] * len(parts),
        out_specs=[ANYWHERE, ANYWHERE],
        scratch_shapes=[
            pltpu.VMEM((blocks, 2 * rank, order), BF16),
            pltpu.VMEM((count, rank, rank), F32),
            pltpu.SemaphoreType.DMA((len(parts),)),
            pltpu.SemaphoreType.DMA((count,)),
            pltpu.SemaphoreType.DMA,
            pltpu.VMEM((count, rank, rank), BF16),
        ],
        out_shape=[
            jax.ShapeDtypeStruct((slots, rank, rank), BF16),
            pltpu.HBM((blocks, rank, order), BF16),
        ],
        compiler_params=params(VMEM_BYTES // 2),
        name="encode",
    )(words, tiles, *parts)


def add_rows(sketch, block, value):
    lanes = sketch.shape[2]
    pieces = value.shape[1] // lanes
    for r in range(pieces):
        sketch[block * pieces + r] += value[:, r * lanes : (r + 1) * lanes]


def prepare_kernel(words, pwords, flip_ref, test_ref, parents, basis_ref, west, vest, sketch, turned):
    blocks, tests = flip_ref.shape[0], test_ref.shape[0]
    count = parents.shape[0]
    sketch[...] = jnp.zeros_like(sketch)
    for b in range(tests):
        turned[b] = test_ref[b].T
    for b in range(blocks):
        basis_ref[b] = flip_ref[b].T

    def parent(p, carry):
        prow, pcol = pwords[2 * p], pwords[2 * p + 1]
        add_rows(
            sketch,
            prow,
            lax.dot_general(turned[pcol], parents[p], NT, preferred_element_type=F32),
        )

        @pl.when(prow != pcol)
        def _():
            add_rows(sketch, pcol, dot(turned[prow], parents[p]))

        return carry

    lax.fori_loop(0, count, parent, 0)

    group = grouped(west.shape[0])

    def item(g, carry):
        for s in [g * group + n for n in range(group)]:
            slot, row, col = unpack(words[s])
            at = 2 * jnp.maximum(slot - 1, 0)
            west[s] = lax.dot_general(
                turned[pwords[at + 1]], flip_ref[col], NT, preferred_element_type=F32
            ).astype(BF16)
            vest[s] = lax.dot_general(
                turned[pwords[at]], flip_ref[row], NT, preferred_element_type=F32
            ).astype(BF16)
        return carry

    lax.fori_loop(0, west.shape[0] // group, item, 0)


def prepare(words, pwords, flipped, test, parents, lanes):
    blocks, rank, order = flipped.shape
    tests, _, width = test.shape
    items = words.shape[0]
    return pl.pallas_call(
        prepare_kernel,
        in_specs=[SCALARS, SCALARS, ON_CHIP, ON_CHIP, ON_CHIP],
        out_specs=[ON_CHIP] * 4,
        scratch_shapes=[pltpu.VMEM((tests, width, order), BF16)],
        out_shape=[
            jax.ShapeDtypeStruct((blocks, order, rank), BF16),
            jax.ShapeDtypeStruct((items, width, rank), BF16),
            jax.ShapeDtypeStruct((items, width, rank), BF16),
            jax.ShapeDtypeStruct((tests * order // lanes, width, lanes), F32),
        ],
        compiler_params=params(VMEM_BYTES),
        cost_estimate=pl.CostEstimate(
            flops=4 * parents.size * width, bytes_accessed=2 * parents.size, transcendentals=0
        ),
        name="prepare",
    )(words, pwords, flipped, test, parents)


def fold_kernel(
    words, pwords, core_ref, west, vest, flip_ref, start, keep_ref, send_ref, sketch, base, sem
):
    base_copy = pltpu.make_async_copy(start, base, sem)
    base_copy.start()
    sketch[...] = jnp.zeros_like(sketch)

    group = grouped(core_ref.shape[0])

    def item(g, carry):
        targets, values = [], []
        for s in [g * group + n for n in range(group)]:
            slot, row, col = unpack(words[s])
            at = 2 * jnp.maximum(slot - 1, 0)
            prow, pcol = pwords[at], pwords[at + 1]
            core = jnp.where(slot > 0, core_ref[s], jnp.zeros_like(core_ref[s]))
            first = lax.dot_general(west[s], core, NT, preferred_element_type=F32)
            second = jnp.where(prow != pcol, dot(vest[s], core), 0.0)
            targets += [prow, pcol]
            values += [(first.astype(BF16), row), (second.astype(BF16), col)]
        values = [dot(value, flip_ref[block]) for value, block in values]
        for target, value in zip(targets, values):
            add_rows(sketch, target, value)
        return carry

    lax.fori_loop(0, core_ref.shape[0] // group, item, 0)
    base_copy.wait()
    core = lax.axis_index("tile") % 2
    for n in range(keep_ref.shape[0]):
        mine, other = 2 * n + core, 2 * n + 1 - core
        keep_ref[n] = (sketch[mine] + base[mine]).astype(BF16)
        send_ref[n] = (sketch[other] + base[other]).astype(BF16)


def fold(words, pwords, cores, west, vest, flipped, start):
    chunks, width, lanes = start.shape
    half = jax.ShapeDtypeStruct((chunks // 2, width, lanes), BF16)
    return pl.pallas_call(
        fold_kernel,
        in_specs=[SCALARS, SCALARS] + [ON_CHIP] * 4 + [ANYWHERE],
        out_specs=[ON_CHIP, ON_CHIP],
        scratch_shapes=[
            pltpu.VMEM(start.shape, F32),
            pltpu.VMEM(start.shape, F32),
            pltpu.SemaphoreType.DMA,
        ],
        out_shape=[half, half],
        compiler_params=params(VMEM_BYTES),
        name="fold",
    )(words, pwords, cores, west, vest, flipped, start)


def update_kernel(
    low, words, parents, partial, core_ref, basis_ref, flip_ref, updated,
    held, total, mixed, made, in_sems, out_sems,
):
    count, items = held.shape[0], core_ref.shape[0]
    group = grouped(items)

    def in_copy(p):
        return pltpu.make_async_copy(parents.at[low + p], held.at[p], in_sems.at[p])

    def out_copy(p):
        return pltpu.make_async_copy(made.at[p], updated.at[low + p], out_sems.at[p])

    for p in range(count):
        in_copy(p).start()

    def mix(g, carry):
        for s in [g * group + n for n in range(group)]:
            _, _, col = unpack(words[s])
            mixed[s] = dot(core_ref[s], flip_ref[col]).astype(BF16)
        return carry

    lax.fori_loop(0, items // group, mix, 0)
    for p in range(count):
        in_copy(p).wait()
        total[p] = held[p].astype(F32)

    def item(s, carry):
        slot, row, _ = unpack(words[s])

        @pl.when((slot > low) & (slot <= low + count))
        def _():
            total[slot - 1 - low] += dot(basis_ref[row], mixed[s])

        return carry

    lax.fori_loop(0, items, item, 0)
    for p in range(count):
        made[p] = total[p].astype(BF16)
        out_copy(p).start()
    for p in range(count):
        out_copy(p).wait()


def update(low, count, words, parents, partial, cores, basis, flipped):
    order = parents.shape[1]
    rank = basis.shape[2]
    items = cores.shape[0]
    first = partial is None
    given = [] if first else [partial]

    def body(words, parents, *refs):
        update_kernel(low, words, parents, *([None] if first else []), *refs)

    return pl.pallas_call(
        body,
        in_specs=[SCALARS, IN_HBM] + [IN_HBM] * len(given) + [ON_CHIP] * 3,
        out_specs=IN_HBM,
        scratch_shapes=[
            pltpu.VMEM((count, order, order), BF16),
            pltpu.VMEM((count, order, order), F32),
            pltpu.VMEM((items, rank, order), BF16),
            pltpu.VMEM((count, order, order), BF16),
            pltpu.SemaphoreType.DMA((count,)),
            pltpu.SemaphoreType.DMA((count,)),
        ],
        out_shape=jax.ShapeDtypeStruct(parents.shape, BF16),
        input_output_aliases={} if first else {2: 0},
        compiler_params=params(),
        cost_estimate=pl.CostEstimate(
            flops=8 * parents.size * rank, bytes_accessed=4 * parents.size, transcendentals=0
        ),
        name="update",
    )(words, parents, *given, cores, basis, flipped)


def partner(i, step, size):
    return i ^ step if size & (size - 1) == 0 else (i + step) % size


def exchange_sum(pieces, size, me, send, group):
    mine = lax.dynamic_slice_in_dim(pieces, me * group, group, 0)
    for shift in range(1, size):
        peer = partner(me, shift, size)
        out = lax.dynamic_slice_in_dim(pieces, peer * group, group, 0).astype(BF16)
        mine = mine + send(out, shift).astype(F32)
    return mine


def reduce_sketch(keep, sent, decode, cores, owners, children):
    child, tile = lax.axis_index("child"), lax.axis_index("tile")
    chips = owners // 2
    pieces = keep.astype(F32) + to_partner(sent, owners).astype(F32)

    def over_child(x, shift):
        return lax.ppermute(
            x, "child", [(i, partner(i, shift, children)) for i in range(children)]
        )

    def over_chips(x, shift):
        return lax.ppermute(
            x, "tile", [(t, 2 * partner(t // 2, shift, chips) + t % 2) for t in range(owners)]
        )

    pieces = exchange_sum(pieces, children, child, over_child, chips)
    pieces, updated, cores = lax.optimization_barrier((pieces, decode(None, cores), cores))
    return exchange_sum(pieces, chips, tile // 2, over_chips, 1)[0], decode(updated, cores)


def shards(
    child_tiles,
    panel,
    bases,
    tile_blocks,
    tile_dest,
    tile_slot,
    parent_tiles,
    parent_blocks,
    sketch_test,
):
    owners, children = lax.axis_size("tile"), lax.axis_size("child")
    myself = lax.axis_index("tile")
    tile_count, order = child_tiles.shape[1], child_tiles.shape[2]

    block = project(panel[0], bases[0], order)
    parts, places, staged = spread(block, child_tiles[0], owners)

    pair_all = pack(0, tile_blocks[0, :, 0], tile_blocks[0, :, 1]).reshape(owners, tile_count)
    dest_all = tile_dest[0, :, 0].reshape(owners, tile_count)
    own_pair = lax.dynamic_index_in_dim(pair_all, myself, 0, keepdims=False)
    own_dest = lax.dynamic_index_in_dim(dest_all, myself, 0, keepdims=False)
    ids = jnp.arange(tile_count, dtype=jnp.int32)
    lower = ids[None, :] < ids[:, None]
    before = (own_dest[:, None] == own_dest[None, :]) & lower
    place = own_dest * CAP + jnp.sum(before.astype(jnp.int32), axis=1)
    own_words = pack(place, 0, own_pair)

    arrive = dest_all == myself
    earlier = jnp.sum((arrive[:, None, :] & lower[None]).astype(jnp.int32), axis=2)
    turn = jnp.arange(CAP, dtype=jnp.int32)
    matched = arrive[:, None, :] & (earlier[:, None, :] == turn[None, :, None])
    word_all = pack(tile_slot[0].reshape(owners, tile_count) + 1, 0, pair_all)
    words = jnp.sum(jnp.where(matched, word_all[:, None, :], 0), axis=2).reshape(-1)
    pwords = parent_blocks[0].reshape(-1)

    cores, flipped = encode(staged, parts, places, own_words, owners)
    rank = cores.shape[1]
    incoming = lax.all_to_all(
        cores.reshape(owners, CAP, rank, rank), "tile", split_axis=0, concat_axis=0, tiled=True
    ).reshape(cores.shape)
    width = sketch_test.shape[1]
    lanes = sketch_test.shape[0] // (owners * children)
    basis, west, vest, start = prepare(
        words, pwords, flipped, sketch_test.reshape(-1, order, width), parent_tiles[0], lanes
    )
    keep, sent = fold(words, pwords, incoming, west, vest, flipped, start)

    def decode(partial, cores):
        count = parent_tiles.shape[1]
        early = count - count // 2
        low, size = (0, early) if partial is None else (early, count - early)
        return update(low, size, words, parent_tiles[0], partial, cores, basis, flipped)

    sketch, updated = reduce_sketch(keep, sent, decode, incoming, owners, children)
    return updated[None], sketch.T


def solution(mesh):
    return jax.shard_map(
        shards,
        mesh=mesh,
        in_specs=(
            P("child", "tile", None, None),
            P("child", "tile", None),
            P("child", "tile", None),
            P("child", None, None),
            P("child", None, None),
            P("child", None),
            P("child", "tile", None, None),
            P("child", "tile", None),
            P(),
        ),
        out_specs=(P("child", "tile", None, None), P(("child", "tile"), None)),
        check_vma=False,
    )
```
